128 devices in a mesh: section: 8 (over x_hi, z), rep: 16 (over x_lo, y, core).
Axes of the slice: x: 4 (x_hi: 2, x_lo: 2; x = x_hi * 2 + x_lo), y: 4, z: 4, core: 2. Of those that a mesh axis runs over, the one named last changes fastest.
Arguments:
- cache: bfloat16 [8, 8192, 3584], P('section', 'rep'), may hold values from -6 to 6
- payload: bfloat16 [8, 8192, 3584], P('section', 'rep'), may hold values from -6 to 6
- block_ids: int32 [8, 16, 2], P('section', 'rep'), may hold values from 0 to 3, as said below
- block_counts: int32 [8, 16], P('section', 'rep'), may hold values from 1 to 2, as said below
- block_scales: int32 [8, 16, 2], P('section', 'rep'), may hold values from 1024 to 8192
- refresh_ids: int32 [8, 16, 128], P('section', 'rep'), may hold values from 0 to 511, as said below
- refresh_counts: int32 [8, 16], P('section', 'rep'), may hold values from 1 to 128, as said below
- norm_gain: float32 [8, 3584], P('section'), may hold values from 0.5 to 1.5
- query_weight: bfloat16 [8, 3584, 3584], P('section', 'rep'), may hold values from -0.09375 to 0.09375
- query_bias: float32 [8, 3584], P('section'), may hold values from -3 to 3
- kv_weight: bfloat16 [8, 3584, 1024], P('section', 'rep'), may hold values from -0.09375 to 0.09375
- kv_bias: float32 [8, 1024], P('section'), may hold values from -3 to 3
Outputs:
- rebuilt: bfloat16 [8, 8192, 3584], P('section', 'rep')
- queries: bfloat16 [8, 8192, 3584], P('section', 'rep')
- keys_values: bfloat16 [8, 8192, 1024], P('section', 'rep')
The draws below stay inside these ranges and needn't reach their ends.
Inputs may be any that keep to these rules, and one draw needn't show every extreme that they name: `block_ids`: for each section and relay the 2 entries are different block numbers; only the first block_counts entries are used. `block_counts`: in every section some relay lists exactly 2 blocks. `refresh_ids`: for each section and relay the entries are different local row numbers; only the first refresh_counts entries are used. `refresh_counts`: in every section some relay lists exactly 128 rows.
All inputs are finite; a program needn't handle non-finite values.
Results may differ from the reference program's by a relative error of at most 0.0052.
Values may be sent and summed in bfloat16 or wider, within the bound.
A program may use at most 256 MiB of HBM per device.

```python
import jax
import jax.numpy as jnp
from jax import lax

D = 3584
QW = 3584
KVW = 1024
BLK = 128
NBLK = 4
MOST_BLK = 2
REF_MAX = 128
ROW_DEV = 512
REPS = 16
SECTIONS = 8
ROWS = 8192


def pick_distinct(key, extent, amount):
    key_list = jax.random.split(key, SECTIONS * REPS)
    chosen = jax.vmap(lambda single: jax.random.permutation(single, extent)[:amount])(key_list)
    return chosen.reshape(SECTIONS, REPS, amount).astype(jnp.int32)


def counts_reaching(key, ceiling):
    front_key, place_key = jax.random.split(key)
    counts = jax.random.randint(front_key, (SECTIONS, REPS), 1, ceiling + 1)
    full_rank = jax.random.randint(place_key, (SECTIONS,), 0, REPS)
    at_full = jnp.arange(REPS)[None, :] == full_rank[:, None]
    return jnp.where(at_full, ceiling, counts).astype(jnp.int32)


def draw_block_ids(key, part):
    return pick_distinct(jax.random.fold_in(key, 11), NBLK, MOST_BLK)


def draw_block_counts(key, part):
    return counts_reaching(jax.random.fold_in(key, 12), MOST_BLK)


def draw_refresh_ids(key, part):
    return pick_distinct(jax.random.fold_in(key, 13), ROW_DEV, REF_MAX)


def draw_refresh_counts(key, part):
    return counts_reaching(jax.random.fold_in(key, 14), REF_MAX)


def touch_ends(values, own_key, low, largest):
    longest = values.shape.index(max(values.shape))
    spots = []
    for shift in (0, 1):
        where = [jax.random.randint(jax.random.fold_in(own_key, axis), (), 0, length) for axis, length in enumerate(values.shape)]
        where[longest] = (where[longest] + shift) % values.shape[longest]
        spots.append(tuple(where))
    return values.at[spots[0]].set(low).at[spots[1]].set(largest)


def level_of(stream_key, dims, pieces, smallest, largest):
    def one(axis_at, blocks):
        heights = jax.random.uniform(jax.random.fold_in(jax.random.fold_in(stream_key, 6), axis_at), (blocks,), jnp.float32, smallest / len(pieces), largest / len(pieces))
        return jnp.repeat(jnp.exp(heights), dims[axis_at] // blocks).reshape((-1,) + (1,) * (len(dims) - axis_at - 1))

    level = one(*pieces[0])
    for cut in pieces[1:]:
        level = level * one(*cut)
    return level


def scatter_about(rng, dims, deviation, bound, cuts=(), kind=jnp.bfloat16):
    entries = deviation * jax.random.normal(rng, dims, jnp.float32)
    if cuts:
        entries = entries * level_of(rng, dims, cuts, -0.22, 0.18)
    return jnp.clip(entries, -bound, bound).astype(kind)


def setup_inputs(seed: int = 0) -> dict:
    keys = jax.random.split(jax.random.key(seed), 13)
    return {
        "cache": scatter_about(keys[0], (SECTIONS, ROWS, D), 1.0, 6.0, ((0, 8), (1, 16))),
        "payload": scatter_about(keys[1], (SECTIONS, ROWS, D), 1.0, 6.0, ((0, 8), (1, 16))),
        "block_ids": draw_block_ids(jax.random.fold_in(keys[12], 71), 0),
        "block_counts": draw_block_counts(jax.random.fold_in(keys[12], 71), 0),
        "block_scales": touch_ends(jax.random.randint(keys[4], (SECTIONS, REPS, MOST_BLK), 1024, 8193), jax.random.fold_in(keys[4], 1), 1024, 8192).astype(jnp.int32),
        "refresh_ids": draw_refresh_ids(jax.random.fold_in(keys[12], 71), 0),
        "refresh_counts": draw_refresh_counts(jax.random.fold_in(keys[12], 71), 0),
        "norm_gain": jnp.clip(1.0 + 0.1 * jax.random.normal(keys[7], (SECTIONS, D), jnp.float32), 0.5, 1.5),
        "query_weight": scatter_about(keys[8], (SECTIONS, D, QW), D ** -0.5, 0.09375, ((0, 8), (1, 16))),
        "query_bias": scatter_about(keys[9], (SECTIONS, QW), 0.5, 3.0, ((0, 8),), jnp.float32),
        "kv_weight": scatter_about(keys[10], (SECTIONS, D, KVW), D ** -0.5, 0.09375, ((0, 8), (1, 16))),
        "kv_bias": scatter_about(keys[11], (SECTIONS, KVW), 0.5, 3.0, ((0, 8),), jnp.float32),
    }


def rebuild(stored, sent, ids, counts, scales, rows_sent, rows_counts):
    stored_blocks = stored.reshape(REPS, NBLK, BLK, D).astype(jnp.float32)
    sent_blocks = sent.reshape(REPS, NBLK, BLK, D).astype(jnp.float32)
    live = jnp.arange(MOST_BLK)[None, :] < counts[:, None]
    factor = jnp.where(live, scales.astype(jnp.float32) / 4096.0, 0.0)
    select = (ids[:, :, None] == jnp.arange(NBLK)[None, None, :]).astype(jnp.float32)
    per_block = lax.optimization_barrier(jnp.sum(factor[:, :, None] * select, axis=1))
    delta = (sent_blocks * per_block[:, :, None, None]).astype(jnp.bfloat16)
    delta = lax.optimization_barrier(delta).astype(jnp.float32)
    mixed = (stored_blocks + delta).reshape(REPS, ROW_DEV, D)
    live_rows = jnp.arange(REF_MAX)[None, :] < rows_counts[:, None]
    matches = (rows_sent[:, :, None] == jnp.arange(ROW_DEV)[None, None, :]) & live_rows[:, :, None]
    hit = jnp.any(matches, axis=1)
    mixed = jnp.where(hit[:, :, None], sent_blocks.reshape(REPS, ROW_DEV, D), mixed)
    return mixed.reshape(REPS * ROW_DEV, D).astype(jnp.bfloat16)

def project(rebuilt_section, gain, query_weight, query_bias, kv_weight, kv_bias):
    wide = rebuilt_section.astype(jnp.float32)
    scale_rows = lax.rsqrt(lax.optimization_barrier(jnp.mean(wide * wide, axis=1, keepdims=True)) + 1e-06)
    normed = (wide * scale_rows * gain[None, :]).astype(jnp.bfloat16)
    queries = jnp.dot(normed, query_weight, preferred_element_type=jnp.float32) + query_bias[None, :]
    keys_values = jnp.dot(normed, kv_weight, preferred_element_type=jnp.float32) + kv_bias[None, :]
    return (queries.astype(jnp.bfloat16), keys_values.astype(jnp.bfloat16))

def reference(cache, payload, block_ids, block_counts, block_scales, refresh_ids, refresh_counts, norm_gain, query_weight, query_bias, kv_weight, kv_bias):
    rebuilt_list = []
    query_list = []
    kv_list = []
    for section in range(SECTIONS):
        if section == 0:
            rebuilt_section = cache[0]
        else:
            rebuilt_section = rebuild(cache[section], payload[section - 1], block_ids[section - 1], block_counts[section - 1], block_scales[section - 1], refresh_ids[section - 1], refresh_counts[section - 1])
        queries, keys_values = project(rebuilt_section, norm_gain[section], query_weight[section], query_bias[section], kv_weight[section], kv_bias[section])
        rebuilt_list.append(rebuilt_section)
        query_list.append(queries)
        kv_list.append(keys_values)
    return (jnp.stack(rebuilt_list), jnp.stack(query_list), jnp.stack(kv_list))
```

```python
import functools

import jax
import jax.numpy as jnp
from jax import lax
from jax.experimental import pallas as pl
from jax.experimental.pallas import tpu as pltpu
from jax.sharding import PartitionSpec as P

EPSILON = 1e-06
BLK = 128
COLS = 256
GRP = 3
MESH = pl.DeviceIdType.MESH

YM, YP, XP, SIB = 0, 1, 2, 3
Y2B, Y2C, Y2A = 4, 5, 6
XYM_BC, XYP_BC, XYP_A, XYM_A = 7, 8, 9, 10
XY2B, XY2C, XY2A = 11, 12, 13
D_YM, D_YP, D_XP, D_Y2, D_XYM, D_XYP, D_XY2 = 14, 15, 16, 17, 18, 19, 20
CLASSES = 21


def kernel(
    cache, payload, meta, gain, q_w, q_b, kv_w, kv_b,
    rebuilt_out, qkv_out,
    wbuf, pay, held, normed, outbuf, relay, meta_in, bias,
    ld_sem, cache_sem, send, recv, pay_send, pay_recv, meta_send, meta_recv,
    relay_send, relay_recv, reb_sem, out_sem,
):
    sec = lax.axis_index("section")
    me = lax.axis_index("rep")
    depth = q_w.shape[0]
    q_blocks = q_w.shape[1] // COLS
    blocks = q_blocks + kv_w.shape[1] // COLS
    groups = blocks // GRP
    row_blocks = payload.shape[0] // BLK

    x, y, core = me // 8, (me // 2) % 4, me % 2

    def rank(dx, dy):
        return ((x + dx) % 2) * 8 + ((y + dy) % 4) * 2 + core

    ym, yp, y2 = rank(0, 3), rank(0, 1), rank(0, 2)
    xp, xym, xyp, xy2 = rank(1, 0), rank(1, 3), rank(1, 1), rank(1, 2)
    other = me + 1 - 2 * core

    def twin(r):
        return r + 1 - 2 * core

    def region(r, first, count):
        rows = pl.ds(pl.multiple_of(r * depth, 32), depth)
        return wbuf.at[pl.ds(first, count), rows, :]

    def remote(ref, cls, g, to):
        return pltpu.make_async_remote_copy(
            src_ref=ref, dst_ref=ref, send_sem=send.at[cls, g], recv_sem=recv.at[cls, g],
            device_id=(sec, to), device_id_type=MESH,
        )

    sent = []

    def push(r, first, count, cls, g, to):
        copy = remote(region(r, first, count), cls, g, to)
        copy.start()
        sent.append(copy)

    def arrive(r, first, count, cls, g):
        remote(region(r, first, count), cls, g, other).wait_recv()

    loads = []
    for j in range(blocks):
        if j < q_blocks:
            src = q_w.at[:, pl.ds(j * COLS, COLS)]
        else:
            src = kv_w.at[:, pl.ds((j - q_blocks) * COLS, COLS)]
        rows = pl.ds(pl.multiple_of(me * depth, 32), depth)
        copy = pltpu.make_async_copy(src, wbuf.at[j, rows, :], ld_sem.at[j])
        copy.start()
        loads.append(copy)

    def block(ref, b):
        return ref.at[pl.ds(b * BLK, BLK), :]

    def pay_copy(src, dst, b, to_sec, to_rep, send_sem, recv_sem):
        return pltpu.make_async_remote_copy(
            src_ref=src, dst_ref=dst, send_sem=send_sem, recv_sem=recv_sem,
            device_id=(to_sec, to_rep), device_id_type=MESH,
        )

    last = lax.axis_size("section") - 1
    half = (last + 1) // 2
    via = (half - 1, last, half, 0)

    def direct(b):
        return pay_copy(block(payload, b), block(pay, b), b, lax.rem(sec + 1, last + 1), me, pay_send.at[b], pay_recv.at[b])

    def first_hop(b):
        return pay_copy(block(payload, b), relay, b, via[b], xp, pay_send.at[b], relay_recv)

    def second_hop(b):
        return pay_copy(relay, block(pay, b), b, half, xp, relay_send, pay_recv.at[b])

    def meta_copy():
        return pay_copy(meta, meta_in, 0, lax.rem(sec + 1, last + 1), me, meta_send, meta_recv)

    @pl.when(sec != last)
    def _():
        meta_copy().start()

    @pl.when(sec == half - 1)
    def _():
        for b in range(row_blocks):
            first_hop(b).start()

    @pl.when((sec != half - 1) & (sec != last))
    def _():
        for b in range(row_blocks):
            direct(b).start()

    fill_meta = pltpu.make_async_copy(meta, meta_in, meta_recv)

    def fill(b):
        return pltpu.make_async_copy(block(payload, b), block(pay, b), pay_recv.at[b])

    @pl.when(sec == 0)
    def _():
        fill_meta.start()
        for b in range(row_blocks):
            fill(b).start()

    load_cache = pltpu.make_async_copy(cache, held, cache_sem)
    load_cache.start()

    for g in range(groups):
        for j in range(g * GRP, (g + 1) * GRP):
            loads[j].wait()
        push(me, g * GRP, GRP, XP, g, xp)
        push(me, g * GRP, GRP, YM, g, yp)
        push(me, g * GRP, GRP, YP, g, ym)
        push(me, g * GRP, GRP, SIB, g, other)

    bias[:, : q_w.shape[1]] = q_b[...]
    bias[:, q_w.shape[1] :] = kv_b[...]

    def level1(g):
        a = g * GRP
        arrive(ym, a, GRP, YM, g)
        push(ym, a + 1, 1, Y2B, g, yp)
        if g % 2 == 0:
            push(ym, a, 1, Y2A, g, yp)
        push(ym, a, 1, XYM_A, g, xp)
        arrive(yp, a, GRP, YP, g)
        push(yp, a + 2, 1, Y2C, g, ym)
        if g % 2 == 1:
            push(yp, a, 1, Y2A, g, ym)
        push(yp, a, 1, XYP_A, g, xp)
        arrive(xp, a, GRP, XP, g)
        push(xp, a + 1, 2, XYM_BC, g, yp)
        push(xp, a + 1, 2, XYP_BC, g, ym)
        push(ym, a, GRP, D_YM, g, other)
        push(yp, a, GRP, D_YP, g, other)
        push(xp, a, GRP, D_XP, g, other)

    def level2(g):
        a = g * GRP
        arrive(xym, a + 1, 2, XYM_BC, g)
        push(xym, a + 1, 1, XY2B, g, yp)
        arrive(xyp, a + 1, 2, XYP_BC, g)
        push(xyp, a + 2, 1, XY2C, g, ym)
        arrive(y2, a, 1, Y2A, g)
        push(y2, a, 1, XY2A, g, xp)
        arrive(y2, a + 1, 1, Y2B, g)
        arrive(y2, a + 2, 1, Y2C, g)
        push(y2, a, GRP, D_Y2, g, other)
        arrive(xym, a, 1, XYM_A, g)
        push(xym, a, GRP, D_XYM, g, other)
        arrive(xyp, a, 1, XYP_A, g)
        push(xyp, a, GRP, D_XYP, g, other)

    def level3(g):
        a = g * GRP
        arrive(xy2, a + 1, 1, XY2B, g)
        arrive(xy2, a + 2, 1, XY2C, g)
        arrive(xy2, a, 1, XY2A, g)
        push(xy2, a, GRP, D_XY2, g, other)

    def relay_step():
        for b in range(row_blocks):
            @pl.when(sec == via[b])
            def _():
                first_hop(b).wait_recv()
                second_hop(b).start()

    valid = sec > 0
    rebuilt_copies = []

    def rebuild(b):
        @pl.when(sec != 0)
        def _():
            direct(b).wait_recv()

        @pl.when(sec == 0)
        def _():
            fill(b).wait()

        lists = meta_in[...]
        lane = lax.broadcasted_iota(jnp.int32, (1, BLK), 1)
        ids = jnp.where((lane < lists[1:2, :]) & valid, lists[0:1, :], -1)
        listed = (lane < lists[4:5, :]) & (lists[2:3, :] == b) & valid
        factor = jnp.sum(jnp.where(listed, lists[3:4, :].astype(jnp.float32) / 4096.0, 0.0), axis=1, keepdims=True)
        strip = 16

        def one(i, carry):
            start = pl.multiple_of(b * BLK + i * strip, strip)
            rows = pl.ds(start, strip)
            number = lax.broadcasted_iota(jnp.int32, (strip, BLK), 0) + start
            hit = jnp.max(jnp.where(number == ids, 1.0, 0.0), axis=1, keepdims=True) > 0.0
            came = pay[rows, :].astype(jnp.float32)
            delta = (came * factor).astype(jnp.bfloat16).astype(jnp.float32)
            mixed = jnp.where(hit, came, held[rows, :].astype(jnp.float32) + delta).astype(jnp.bfloat16)
            held[rows, :] = mixed
            wide = mixed.astype(jnp.float32)
            scale = lax.rsqrt(jnp.mean(wide * wide, axis=1, keepdims=True) + EPSILON)
            normed[rows, :] = (wide * scale * gain[...]).astype(jnp.bfloat16)
            return carry

        lax.fori_loop(0, BLK // strip, one, 0)
        copy = pltpu.make_async_copy(block(held, b), block(rebuilt_out, b), reb_sem.at[b])
        copy.start()
        rebuilt_copies.append(copy)

    def out_copy(j):
        cols = pl.ds(pl.multiple_of(j * COLS, COLS), COLS)
        return pltpu.make_async_copy(outbuf.at[j], qkv_out.at[:, cols], out_sem.at[j])

    def compute(g):
        a = g * GRP
        for r, cls in ((me, SIB), (ym, D_YM), (yp, D_YP), (xp, D_XP), (y2, D_Y2), (xym, D_XYM), (xyp, D_XYP), (xy2, D_XY2)):
            arrive(twin(r), a, GRP, cls, g)

        def one(j, carry):
            total = jnp.dot(normed[...], wbuf[j], preferred_element_type=jnp.float32)
            cols = pl.ds(pl.multiple_of(j * COLS, COLS), COLS)
            outbuf[j] = (total + bias[:, cols]).astype(jnp.bfloat16)
            out_copy(j).start()
            return carry

        lax.fori_loop(a, a + GRP, one, 0)

    level1(0)
    level1(1)
    load_cache.wait()

    @pl.when(sec != 0)
    def _():
        meta_copy().wait_recv()

    @pl.when(sec == 0)
    def _():
        fill_meta.wait()

    relay_step()
    rebuild(0)
    rebuild(1)
    level2(0)
    level1(2)
    rebuild(2)
    level2(1)
    level3(0)
    level1(3)
    level2(2)
    level3(1)
    level1(4)
    rebuild(3)
    level2(3)
    level3(2)
    level1(5)
    compute(0)
    compute(1)
    level2(4)
    level3(3)
    compute(2)
    compute(3)
    level2(5)
    level3(4)
    compute(4)
    level3(5)
    compute(5)

    for copy in sent:
        copy.wait_send()
    for copy in rebuilt_copies:
        copy.wait()
    for j in range(blocks):
        out_copy(j).wait()

    @pl.when(sec != last)
    def _():
        meta_copy().wait_send()
        for b in range(row_blocks):
            direct(b).wait_send()

    for b in range(row_blocks):
        @pl.when(sec == via[b])
        def _():
            second_hop(b).wait_send()


def body(
    cache, payload, block_ids, block_counts, block_scales, refresh_ids, refresh_counts,
    norm_gain, query_weight, query_bias, kv_weight, kv_bias,
):
    rows, feature = cache.shape[1:]
    depth, q_cols = query_weight.shape[1:]
    kv_cols = kv_weight.shape[2]
    blocks = (q_cols + kv_cols) // COLS
    groups = blocks // GRP
    row_blocks = rows // BLK

    def lanes(v):
        return jnp.pad(v.reshape(1, -1), ((0, 0), (0, BLK - v.size)))

    meta = jnp.concatenate(
        [
            lanes(refresh_ids[0, 0]),
            jnp.broadcast_to(refresh_counts[0, 0], (1, BLK)),
            lanes(block_ids[0, 0]),
            lanes(block_scales[0, 0]),
            jnp.broadcast_to(block_counts[0, 0], (1, BLK)),
            jnp.zeros((3, BLK), jnp.int32),
        ],
        axis=0,
    )
    anywhere = pl.BlockSpec(memory_space=pl.ANY)
    vmem = pl.BlockSpec(memory_space=pltpu.VMEM)
    dma = pltpu.SemaphoreType.DMA
    rebuilt, qkv = pl.pallas_call(
        kernel,
        out_shape=(
            jax.ShapeDtypeStruct((rows, feature), jnp.bfloat16),
            jax.ShapeDtypeStruct((rows, q_cols + kv_cols), jnp.bfloat16),
        ),
        in_specs=[anywhere, anywhere, anywhere, vmem, anywhere, vmem, anywhere, vmem],
        out_specs=(anywhere, anywhere),
        scratch_shapes=[
            pltpu.VMEM((blocks, feature, COLS), jnp.bfloat16),
            pltpu.VMEM((rows, feature), jnp.bfloat16),
            pltpu.VMEM((rows, feature), jnp.bfloat16),
            pltpu.VMEM((rows, feature), jnp.bfloat16),
            pltpu.VMEM((blocks, rows, COLS), jnp.bfloat16),
            pltpu.VMEM((BLK, feature), jnp.bfloat16),
            pltpu.VMEM((8, BLK), jnp.int32),
            pltpu.VMEM((1, q_cols + kv_cols), jnp.float32),
            dma((blocks,)),
            dma,
            dma((CLASSES, groups)),
            dma((CLASSES, groups)),
            dma((row_blocks,)),
            dma((row_blocks,)),
            dma,
            dma,
            dma,
            dma,
            dma((row_blocks,)),
            dma((blocks,)),
        ],
        compiler_params=pltpu.CompilerParams(has_side_effects=True, vmem_limit_bytes=64 * 1024 * 1024 - 65536),
        name="boundary",
    )(cache[0], payload[0], meta, norm_gain, query_weight[0], query_bias, kv_weight[0], kv_bias)
    return rebuilt[None], qkv[None, :, :q_cols], qkv[None, :, q_cols:]


def solution(mesh):
    in_specs = (
        P("section", "rep", None),
        P("section", "rep", None),
        P("section", "rep", None),
        P("section", "rep"),
        P("section", "rep", None),
        P("section", "rep", None),
        P("section", "rep"),
        P("section", None),
        P("section", "rep", None),
        P("section", None),
        P("section", "rep", None),
        P("section", None),
    )
    out_specs = (P("section", "rep", None), P("section", "rep", None), P("section", "rep", None))
    return jax.shard_map(body, mesh=mesh, in_specs=in_specs, out_specs=out_specs, check_vma=False)
```

```python
import functools

import jax
import jax.numpy as jnp
from jax import lax
from jax.experimental import pallas as pl
from jax.experimental.pallas import tpu as pltpu
from jax.sharding import PartitionSpec as P

EPSILON = 1e-06
BLK = 128
COLS = 256
GRP = 3
MESH = pl.DeviceIdType.MESH

YM, YP, XP, SIB = 0, 1, 2, 3
Y2B, Y2C, Y2A = 4, 5, 6
XYM_BC, XYP_BC, XYP_A, XYM_A = 7, 8, 9, 10
XY2B, XY2C, XY2A = 11, 12, 13
D_YM, D_YP, D_XP, D_Y2, D_XYM, D_XYP, D_XY2 = 14, 15, 16, 17, 18, 19, 20
CLASSES = 21


def kernel(
    cache, payload, ids, counts, scales, refresh_ids, refresh_counts, gain, q_w, q_b, kv_w, kv_b,
    rebuilt_out, q_out, kv_out,
    wbuf, pay, held, normed, outbuf, relay, relay_two, meta, meta_in, bias,
    ld_sem, cache_sem, send, recv, pay_send, pay_recv, meta_send, meta_recv,
    relay_send, relay_recv, two_send, two_recv, reb_sem, out_sem,
):
    sec = lax.axis_index("section")
    me = lax.axis_index("rep")
    depth = q_w.shape[0]
    q_blocks = q_w.shape[1] // COLS
    blocks = q_blocks + kv_w.shape[1] // COLS
    groups = blocks // GRP
    row_blocks = payload.shape[0] // BLK

    x, y, core = me // 8, (me // 2) % 4, me % 2

    def rank(dx, dy):
        return ((x + dx) % 2) * 8 + ((y + dy) % 4) * 2 + core

    ym, yp, y2 = rank(0, 3), rank(0, 1), rank(0, 2)
    xp, xym, xyp, xy2 = rank(1, 0), rank(1, 3), rank(1, 1), rank(1, 2)
    other = me + 1 - 2 * core

    def twin(r):
        return r + 1 - 2 * core

    def region(r, first, count):
        rows = pl.ds(pl.multiple_of(r * depth, 32), depth)
        return wbuf.at[pl.ds(first, count), rows, :]

    def remote(ref, cls, g, to):
        return pltpu.make_async_remote_copy(
            src_ref=ref, dst_ref=ref, send_sem=send.at[cls, g], recv_sem=recv.at[cls, g],
            device_id=(sec, to), device_id_type=MESH,
        )

    sent = []

    def push(r, first, count, cls, g, to):
        copy = remote(region(r, first, count), cls, g, to)
        copy.start()
        sent.append(copy)

    def arrive(r, first, count, cls, g):
        remote(region(r, first, count), cls, g, other).wait_recv()

    loads = []
    for j in range(blocks):
        if j < q_blocks:
            src = q_w.at[:, pl.ds(j * COLS, COLS)]
        else:
            src = kv_w.at[:, pl.ds((j - q_blocks) * COLS, COLS)]
        rows = pl.ds(pl.multiple_of(me * depth, 32), depth)
        copy = pltpu.make_async_copy(src, wbuf.at[j, rows, :], ld_sem.at[j])
        copy.start()
        loads.append(copy)

    lane = lax.broadcasted_iota(jnp.int32, (1, BLK), 1)

    def two(v):
        return jnp.where(lane == 0, v[:, 0:1], v[:, 1:2])

    meta[0:1, :] = refresh_ids[...]
    meta[1:2, :] = jnp.broadcast_to(refresh_counts[...], (1, BLK))
    meta[2:3, :] = two(ids[...])
    meta[3:4, :] = two(scales[...])
    meta[4:5, :] = jnp.broadcast_to(counts[...], (1, BLK))
    meta[5:8, :] = jnp.zeros((3, BLK), jnp.int32)

    load_cache = pltpu.make_async_copy(cache, held, cache_sem)
    load_cache.start()

    last = lax.axis_size("section") - 1
    half = (last + 1) // 2
    barrier = pltpu.get_barrier_semaphore()

    def greet(to_sec, to_rep):
        pl.semaphore_signal(barrier, inc=1, device_id=(to_sec, to_rep), device_id_type=MESH)

    for r in (ym, yp, xp, other):
        greet(sec, r)
    expected = 4
    pairs = [(s, s + 1, me) for s in range(last)]
    pairs += [(0, half - 1, me), (half - 1, last, xp), (half - 1, half, xp), (half, last, xp), (0, half, xp)]
    for one, two, r in pairs:
        @pl.when(sec == one)
        def _():
            greet(two, r)

        @pl.when(sec == two)
        def _():
            greet(one, r)

        expected = expected + jnp.where((sec == one) | (sec == two), 1, 0)
    pl.semaphore_wait(barrier, expected)

    def block(ref, b):
        return ref.at[pl.ds(b * BLK, BLK), :]

    def pay_copy(src, dst, to_sec, to_rep, send_sem, recv_sem):
        return pltpu.make_async_remote_copy(
            src_ref=src, dst_ref=dst, send_sem=send_sem, recv_sem=recv_sem,
            device_id=(to_sec, to_rep), device_id_type=MESH,
        )

    following = lax.rem(sec + 1, last + 1)
    via = (half, half - 1, last, 0)

    def direct(b):
        return pay_copy(block(payload, b), block(pay, b), following, me, pay_send.at[b], pay_recv.at[b])

    def first_hop(b):
        return pay_copy(block(payload, b), relay, via[b], xp if via[b] else me, pay_send.at[b], relay_recv)

    def middle_hop():
        return pay_copy(relay, relay_two, 0, xp, relay_send, two_recv)

    def last_hop(b):
        src, sem = (relay, relay_send) if via[b] else (relay_two, two_send)
        return pay_copy(src, block(pay, b), half, xp, sem, pay_recv.at[b])

    def relay_step(b):
        @pl.when(sec == via[b])
        def _():
            first_hop(b).wait_recv()
            (last_hop(b) if via[b] else middle_hop()).start()

    def relay_end(b):
        @pl.when(sec == 0)
        def _():
            middle_hop().wait_recv()
            last_hop(b).start()

    def meta_copy():
        return pay_copy(meta, meta_in, following, me, meta_send, meta_recv)

    @pl.when(sec != last)
    def _():
        meta_copy().start()

    @pl.when(sec == half - 1)
    def _():
        for b in (0, 2, 3):
            first_hop(b).start()

    @pl.when((sec != half - 1) & (sec != last))
    def _():
        for b in range(row_blocks):
            direct(b).start()

    def fill(b):
        return pltpu.make_async_copy(block(payload, b), block(pay, b), pay_recv.at[b])

    @pl.when(sec == 0)
    def _():
        meta_in[...] = jnp.zeros((8, BLK), jnp.int32)
        for b in range(row_blocks):
            fill(b).start()

    def own_x(g):
        push(me, g * GRP, GRP, XP, g, xp)

    for g in range(groups):
        for j in range(g * GRP, (g + 1) * GRP):
            loads[j].wait()
        push(me, g * GRP, GRP, YM, g, yp)
        push(me, g * GRP, GRP, YP, g, ym)
        if g < groups // 2:
            own_x(g)
        if g == 1:
            @pl.when(sec == half - 1)
            def _():
                first_hop(1).start()

        push(me, g * GRP, GRP, SIB, g, other)

    bias[:, : q_w.shape[1]] = q_b[...]
    bias[:, q_w.shape[1] :] = kv_b[...]

    def level1(g):
        a = g * GRP
        arrive(xp, a, GRP, XP, g)
        push(xp, a + 1, 2, XYM_BC, g, yp)
        push(xp, a + 1, 2, XYP_BC, g, ym)
        push(xp, a, GRP, D_XP, g, other)
        arrive(ym, a, GRP, YM, g)
        push(ym, a + 1, 1, Y2B, g, yp)
        if g % 2 == 0:
            push(ym, a, 1, Y2A, g, yp)
        push(ym, a, 1, XYM_A, g, xp)
        push(ym, a, GRP, D_YM, g, other)
        arrive(yp, a, GRP, YP, g)
        push(yp, a + 2, 1, Y2C, g, ym)
        if g % 2 == 1:
            push(yp, a, 1, Y2A, g, ym)
        push(yp, a, 1, XYP_A, g, xp)
        push(yp, a, GRP, D_YP, g, other)

    def level2(g):
        a = g * GRP
        arrive(xym, a + 1, 2, XYM_BC, g)
        push(xym, a + 1, 1, XY2B, g, yp)
        arrive(xyp, a + 1, 2, XYP_BC, g)
        push(xyp, a + 2, 1, XY2C, g, ym)
        arrive(y2, a, 1, Y2A, g)
        push(y2, a, 1, XY2A, g, xp)
        arrive(y2, a + 1, 1, Y2B, g)
        arrive(y2, a + 2, 1, Y2C, g)
        push(y2, a, GRP, D_Y2, g, other)
        arrive(xym, a, 1, XYM_A, g)
        push(xym, a, GRP, D_XYM, g, other)
        arrive(xyp, a, 1, XYP_A, g)
        push(xyp, a, GRP, D_XYP, g, other)

    def level3(g):
        a = g * GRP
        arrive(xy2, a + 1, 1, XY2B, g)
        arrive(xy2, a + 2, 1, XY2C, g)
        arrive(xy2, a, 1, XY2A, g)
        push(xy2, a, GRP, D_XY2, g, other)

    valid = sec > 0
    rebuilt_copies = []

    def rebuild(b):
        @pl.when(sec != 0)
        def _():
            direct(b).wait_recv()

        @pl.when(sec == 0)
        def _():
            fill(b).wait()

        lists = meta_in[...]
        refreshed = jnp.where((lane < lists[1:2, :]) & valid, lists[0:1, :], -1)
        listed = (lane < lists[4:5, :]) & (lane < ids.shape[1]) & (lists[2:3, :] == b) & valid
        factor = jnp.sum(jnp.where(listed, lists[3:4, :].astype(jnp.float32) / 4096.0, 0.0), axis=1, keepdims=True)
        strip = 16

        def one(i, carry):
            start = pl.multiple_of(b * BLK + i * strip, strip)
            rows = pl.ds(start, strip)
            number = lax.broadcasted_iota(jnp.int32, (strip, BLK), 0) + start
            hit = jnp.max(jnp.where(number == refreshed, 1.0, 0.0), axis=1, keepdims=True) > 0.0
            came = pay[rows, :].astype(jnp.float32)
            delta = (came * factor).astype(jnp.bfloat16).astype(jnp.float32)
            mixed = jnp.where(hit, came, held[rows, :].astype(jnp.float32) + delta).astype(jnp.bfloat16)
            held[rows, :] = mixed
            wide = mixed.astype(jnp.float32)
            scale = lax.rsqrt(jnp.mean(wide * wide, axis=1, keepdims=True) + EPSILON)
            normed[rows, :] = (wide * scale * gain[...]).astype(jnp.bfloat16)
            return carry

        lax.fori_loop(0, BLK // strip, one, 0)
        copy = pltpu.make_async_copy(block(held, b), block(rebuilt_out, b), reb_sem.at[b])
        copy.start()
        rebuilt_copies.append(copy)

    def out_copy(j):
        out, k = (q_out, j) if j < q_blocks else (kv_out, j - q_blocks)
        return pltpu.make_async_copy(outbuf.at[j], out.at[:, pl.ds(k * COLS, COLS)], out_sem.at[j])

    def compute(g):
        a = g * GRP
        for r, cls in ((me, SIB), (ym, D_YM), (yp, D_YP), (xp, D_XP), (y2, D_Y2), (xym, D_XYM), (xyp, D_XYP), (xy2, D_XY2)):
            arrive(twin(r), a, GRP, cls, g)

        def one(j, carry):
            total = jnp.dot(normed[...], wbuf[j], preferred_element_type=jnp.float32)
            cols = pl.ds(pl.multiple_of(j * COLS, COLS), COLS)
            outbuf[j] = (total + bias[:, cols]).astype(jnp.bfloat16)
            return carry

        lax.fori_loop(a, a + GRP, one, 0)
        for j in range(a, a + GRP):
            out_copy(j).start()

    level1(0)
    level1(1)
    relay_step(0)
    relay_step(3)
    for g in range(groups // 2, groups):
        own_x(g)
    load_cache.wait()

    @pl.when(sec != 0)
    def _():
        meta_copy().wait_recv()

    relay_step(1)
    relay_step(2)
    level2(0)
    level1(2)
    relay_end(3)
    rebuild(0)
    level2(1)
    level3(0)
    level1(3)
    rebuild(1)
    level2(2)
    level3(1)
    level1(4)
    rebuild(2)
    rebuild(3)
    compute(0)
    level2(3)
    level3(2)
    level1(5)
    compute(1)
    compute(2)
    level2(4)
    level3(3)
    compute(3)
    level3(4)
    compute(4)
    level2(5)
    level3(5)
    compute(5)

    for copy in sent:
        copy.wait_send()
    for copy in rebuilt_copies:
        copy.wait()
    for j in range(blocks):
        out_copy(j).wait()

    @pl.when(sec != last)
    def _():
        meta_copy().wait_send()
        for b in range(row_blocks):
            direct(b).wait_send()

    for b in range(row_blocks):
        @pl.when(sec == via[b])
        def _():
            (last_hop(b) if via[b] else middle_hop()).wait_send()

    @pl.when(sec == 0)
    def _():
        last_hop(3).wait_send()


def body(
    cache, payload, block_ids, block_counts, block_scales, refresh_ids, refresh_counts,
    norm_gain, query_weight, query_bias, kv_weight, kv_bias,
):
    rows, feature = cache.shape[1:]
    depth, q_cols = query_weight.shape[1:]
    kv_cols = kv_weight.shape[2]
    blocks = (q_cols + kv_cols) // COLS
    groups = blocks // GRP
    row_blocks = rows // BLK

    anywhere = pl.BlockSpec(memory_space=pl.ANY)
    vmem = pl.BlockSpec(memory_space=pltpu.VMEM)
    dma = pltpu.SemaphoreType.DMA
    rebuilt, queries, keys_values = pl.pallas_call(
        kernel,
        out_shape=(
            jax.ShapeDtypeStruct((rows, feature), jnp.bfloat16),
            jax.ShapeDtypeStruct((rows, q_cols), jnp.bfloat16),
            jax.ShapeDtypeStruct((rows, kv_cols), jnp.bfloat16),
        ),
        in_specs=[anywhere, anywhere, vmem, vmem, vmem, vmem, vmem, vmem, anywhere, vmem, anywhere, vmem],
        out_specs=(anywhere, anywhere, anywhere),
        scratch_shapes=[
            pltpu.VMEM((blocks, feature, COLS), jnp.bfloat16),
            pltpu.VMEM((rows, feature), jnp.bfloat16),
            pltpu.VMEM((rows, feature), jnp.bfloat16),
            pltpu.VMEM((rows, feature), jnp.bfloat16),
            pltpu.VMEM((blocks, rows, COLS), jnp.bfloat16),
            pltpu.VMEM((BLK, feature), jnp.bfloat16),
            pltpu.VMEM((BLK, feature), jnp.bfloat16),
            pltpu.VMEM((8, BLK), jnp.int32),
            pltpu.VMEM((8, BLK), jnp.int32),
            pltpu.VMEM((1, q_cols + kv_cols), jnp.float32),
            dma((blocks,)),
            dma,
            dma((CLASSES, groups)),
            dma((CLASSES, groups)),
            dma((row_blocks,)),
            dma((row_blocks,)),
            dma,
            dma,
            dma,
            dma,
            dma,
            dma,
            dma((row_blocks,)),
            dma((blocks,)),
        ],
        compiler_params=pltpu.CompilerParams(collective_id=0, has_side_effects=True, vmem_limit_bytes=64 * 1024 * 1024 - 65536),
        name="boundary",
    )(
        cache[0], payload[0], block_ids[0], block_counts, block_scales[0], refresh_ids[0], refresh_counts,
        norm_gain, query_weight[0], query_bias, kv_weight[0], kv_bias,
    )
    return rebuilt[None], queries[None], keys_values[None]


def solution(mesh):
    in_specs = (
        P("section", "rep", None),
        P("section", "rep", None),
        P("section", "rep", None),
        P("section", "rep"),
        P("section", "rep", None),
        P("section", "rep", None),
        P("section", "rep"),
        P("section", None),
        P("section", "rep", None),
        P("section", None),
        P("section", "rep", None),
        P("section", None),
    )
    out_specs = (P("section", "rep", None), P("section", "rep", None), P("section", "rep", None))
    return jax.shard_map(body, mesh=mesh, in_specs=in_specs, out_specs=out_specs, check_vma=False)
```

```python
import functools

import jax
import jax.numpy as jnp
from jax import lax
from jax.experimental import pallas as pl
from jax.experimental.pallas import tpu as pltpu
from jax.sharding import PartitionSpec as P

EPSILON = 1e-06
BLK = 128
COLS = 256
GRP = 3
MESH = pl.DeviceIdType.MESH

YM, YP, XP, SIB = 0, 1, 2, 3
Y2B, Y2C, Y2A = 4, 5, 6
XYM_BC, XYP_BC, XYP_A, XYM_A = 7, 8, 9, 10
XY2B, XY2C, XY2A = 11, 12, 13
D_YM, D_YP, D_XP, D_Y2, D_XYM, D_XYP, D_XY2 = 14, 15, 16, 17, 18, 19, 20
D_XYM_A, D_XYP_A, D_XY2_A = 21, 22, 23
CLASSES = 24


def kernel(
    cache, payload, ids, counts, scales, refresh_ids, refresh_counts, gain, q_w, q_b, kv_w, kv_b,
    rebuilt_out, q_out, kv_out,
    wbuf, pay, held, normed, outbuf, partial, relay, relay_two, relay_three, meta, meta_in, bias,
    ld_sem, cache_sem, send, recv, pay_send, pay_recv, meta_send, meta_recv,
    relay_send, relay_recv, two_send, two_recv, three_send, three_recv, reb_sem, out_sem,
):
    sec = lax.axis_index("section")
    me = lax.axis_index("rep")
    depth = q_w.shape[0]
    q_blocks = q_w.shape[1] // COLS
    blocks = q_blocks + kv_w.shape[1] // COLS
    groups = blocks // GRP
    row_blocks = payload.shape[0] // BLK

    x, y, core = me // 8, (me // 2) % 4, me % 2

    def rank(dx, dy):
        return ((x + dx) % 2) * 8 + ((y + dy) % 4) * 2 + core

    ym, yp, y2 = rank(0, 3), rank(0, 1), rank(0, 2)
    xp, xym, xyp, xy2 = rank(1, 0), rank(1, 3), rank(1, 1), rank(1, 2)
    other = me + 1 - 2 * core

    def twin(r):
        return r + 1 - 2 * core

    def region(r, first, count):
        rows = pl.ds(pl.multiple_of(r * depth, 32), depth)
        return wbuf.at[pl.ds(first, count), rows, :]

    def remote(ref, cls, g, to):
        return pltpu.make_async_remote_copy(
            src_ref=ref, dst_ref=ref, send_sem=send, recv_sem=recv.at[cls, g],
            device_id=(sec, to), device_id_type=MESH,
        )

    sent = []

    def push(r, first, count, cls, g, to):
        copy = remote(region(r, first, count), cls, g, to)
        copy.start()
        sent.append(count)

    def arrive(r, first, count, cls, g):
        remote(region(r, first, count), cls, g, other).wait_recv()

    loads = []
    for j in range(blocks):
        if j < q_blocks:
            src = q_w.at[:, pl.ds(j * COLS, COLS)]
        else:
            src = kv_w.at[:, pl.ds((j - q_blocks) * COLS, COLS)]
        rows = pl.ds(pl.multiple_of(me * depth, 32), depth)
        copy = pltpu.make_async_copy(src, wbuf.at[j, rows, :], ld_sem.at[j])
        copy.start()
        loads.append(copy)

    lane = lax.broadcasted_iota(jnp.int32, (1, BLK), 1)

    def two(v):
        return jnp.where(lane == 0, v[:, 0:1], v[:, 1:2])

    meta[0:1, :] = refresh_ids[...]
    meta[1:2, :] = jnp.broadcast_to(refresh_counts[...], (1, BLK))
    meta[2:3, :] = two(ids[...])
    meta[3:4, :] = two(scales[...])
    meta[4:5, :] = jnp.broadcast_to(counts[...], (1, BLK))
    meta[5:8, :] = jnp.zeros((3, BLK), jnp.int32)

    load_cache = pltpu.make_async_copy(cache, held, cache_sem)
    load_cache.start()

    last = lax.axis_size("section") - 1
    half = (last + 1) // 2
    barrier = pltpu.get_barrier_semaphore()

    def greet(to_sec, to_rep):
        pl.semaphore_signal(barrier, inc=1, device_id=(to_sec, to_rep), device_id_type=MESH)

    for r in (ym, yp, xp, other):
        greet(sec, r)
    expected = 4
    pairs = [(s, s + 1, me) for s in range(last)]
    pairs += [(0, half - 1, me), (half - 1, last, xp), (half - 1, half, xp), (half, last, xp), (0, half, xp)]
    for one, two, r in pairs:
        @pl.when(sec == one)
        def _():
            greet(two, r)

        @pl.when(sec == two)
        def _():
            greet(one, r)

        expected = expected + jnp.where((sec == one) | (sec == two), 1, 0)
    pl.semaphore_wait(barrier, expected)

    def block(ref, b):
        return ref.at[pl.ds(b * BLK, BLK), :]

    def pay_copy(src, dst, to_sec, to_rep, send_sem, recv_sem):
        return pltpu.make_async_remote_copy(
            src_ref=src, dst_ref=dst, send_sem=send_sem, recv_sem=recv_sem,
            device_id=(to_sec, to_rep), device_id_type=MESH,
        )

    following = lax.rem(sec + 1, last + 1)

    def direct(b):
        return pay_copy(block(payload, b), block(pay, b), following, me, pay_send.at[b], pay_recv.at[b])

    def first_hop(b):
        to_sec, to_rep = ((last, xp), (half - 1, xp), (0, me), (0, me))[b]
        dst, sem = (relay_two, two_recv) if b == 3 else (relay, relay_recv)
        return pay_copy(block(payload, b), dst, to_sec, to_rep, pay_send.at[b], sem)

    def over():
        return pay_copy(relay, relay, half, xp, relay_send, relay_recv)

    def across():
        return pay_copy(relay_two, relay_three, 0, xp, two_send, three_recv)

    def last_hop(b):
        src, sem = (relay_three, three_send) if b == 3 else (relay, relay_send)
        return pay_copy(src, block(pay, b), half, xp, sem, pay_recv.at[b])

    def relay_first():
        @pl.when(sec == last)
        def _():
            first_hop(0).wait_recv()
            last_hop(0).start()

        @pl.when(sec == 0)
        def _():
            first_hop(2).wait_recv()
            over().start()

    def relay_second():
        @pl.when(sec == half - 1)
        def _():
            first_hop(1).wait_recv()
            last_hop(1).start()

        @pl.when(sec == half)
        def _():
            over().wait_recv()
            last_hop(2).start()

        @pl.when(sec == 0)
        def _():
            first_hop(3).wait_recv()
            across().start()

    def relay_third():
        @pl.when(sec == 0)
        def _():
            across().wait_recv()
            last_hop(3).start()

    def meta_copy():
        return pay_copy(meta, meta_in, following, me, meta_send, meta_recv)

    @pl.when(sec != last)
    def _():
        meta_copy().start()

    @pl.when(sec == half - 1)
    def _():
        for b in (0, 2, 3):
            first_hop(b).start()

    @pl.when((sec != half - 1) & (sec != last))
    def _():
        for b in range(row_blocks):
            direct(b).start()

    def fill(b):
        return pltpu.make_async_copy(block(payload, b), block(pay, b), pay_recv.at[b])

    @pl.when(sec == 0)
    def _():
        meta_in[...] = jnp.zeros((8, BLK), jnp.int32)
        for b in range(row_blocks):
            fill(b).start()

    def own_x(g):
        push(me, g * GRP, GRP, XP, g, xp)

    for g in range(groups):
        for j in range(g * GRP, (g + 1) * GRP):
            loads[j].wait()
        push(me, g * GRP, GRP, YM, g, yp)
        push(me, g * GRP, GRP, YP, g, ym)
        if g < groups // 2:
            own_x(g)
        if g == 1:
            @pl.when(sec == half - 1)
            def _():
                first_hop(1).start()

        push(me, g * GRP, GRP, SIB, g, other)

    bias[:, : q_w.shape[1]] = q_b[...]
    bias[:, q_w.shape[1] :] = kv_b[...]

    def level1(g):
        a = g * GRP
        there, source = (yp, ym) if g % 2 == 0 else (ym, yp)
        final = g == groups - 1
        arrive(ym, a, GRP, YM, g)
        arrive(yp, a, GRP, YP, g)
        if final:
            push(source, a, 1, Y2A, g, there)
        arrive(xp, a, GRP, XP, g)
        push(xp, a + 1, 2, XYM_BC, g, yp)
        push(xp, a + 1, 2, XYP_BC, g, ym)
        push(ym, a + 1, 1, Y2B, g, yp)
        push(yp, a + 2, 1, Y2C, g, ym)
        if not final:
            push(source, a, 1, Y2A, g, there)
        push(xp, a, GRP, D_XP, g, other)
        push(ym, a, GRP, D_YM, g, other)
        push(yp, a, GRP, D_YP, g, other)

    def beside(g):
        push(ym, g * GRP, 1, XYM_A, g, xp)
        push(yp, g * GRP, 1, XYP_A, g, xp)

    def level2(g):
        a = g * GRP
        arrive(xym, a + 1, 2, XYM_BC, g)
        push(xym, a + 1, 1, XY2B, g, yp)
        arrive(xyp, a + 1, 2, XYP_BC, g)
        push(xyp, a + 2, 1, XY2C, g, ym)
        push(xym, a + 1, 2, D_XYM, g, other)
        push(xyp, a + 1, 2, D_XYP, g, other)

    def opposite_a(g):
        arrive(y2, g * GRP, 1, Y2A, g)
        push(y2, g * GRP, 1, XY2A, g, xp)

    def opposite(g):
        a = g * GRP
        arrive(y2, a + 1, 1, Y2B, g)
        arrive(y2, a + 2, 1, Y2C, g)
        push(y2, a, GRP, D_Y2, g, other)

    def far(g):
        a = g * GRP
        arrive(xy2, a + 1, 1, XY2B, g)
        arrive(xy2, a + 2, 1, XY2C, g)
        push(xy2, a + 1, 2, D_XY2, g, other)

    def sides(g):
        a = g * GRP
        arrive(xym, a, 1, XYM_A, g)
        push(xym, a, 1, D_XYM_A, g, other)
        arrive(xyp, a, 1, XYP_A, g)
        push(xyp, a, 1, D_XYP_A, g, other)
        arrive(xy2, a, 1, XY2A, g)
        push(xy2, a, 1, D_XY2_A, g, other)

    valid = sec > 0
    rebuilt_copies = []

    def rebuild(b):
        @pl.when(sec != 0)
        def _():
            direct(b).wait_recv()

        @pl.when(sec == 0)
        def _():
            fill(b).wait()

        lists = meta_in[...]
        refreshed = jnp.where((lane < lists[1:2, :]) & valid, lists[0:1, :], -1)
        listed = (lane < lists[4:5, :]) & (lane < ids.shape[1]) & (lists[2:3, :] == b) & valid
        factor = jnp.sum(jnp.where(listed, lists[3:4, :].astype(jnp.float32) / 4096.0, 0.0), axis=1, keepdims=True)
        strip = 16

        def one(i, carry):
            start = pl.multiple_of(b * BLK + i * strip, strip)
            rows = pl.ds(start, strip)
            number = lax.broadcasted_iota(jnp.int32, (strip, BLK), 0) + start
            hit = jnp.max(jnp.where(number == refreshed, 1.0, 0.0), axis=1, keepdims=True) > 0.0
            came = pay[rows, :].astype(jnp.float32)
            delta = (came * factor).astype(jnp.bfloat16).astype(jnp.float32)
            mixed = jnp.where(hit, came, held[rows, :].astype(jnp.float32) + delta).astype(jnp.bfloat16)
            held[rows, :] = mixed
            wide = mixed.astype(jnp.float32)
            scale = lax.rsqrt(jnp.mean(wide * wide, axis=1, keepdims=True) + EPSILON)
            normed[rows, :] = (wide * scale * gain[...]).astype(jnp.bfloat16)
            return carry

        lax.fori_loop(0, BLK // strip, one, 0)
        copy = pltpu.make_async_copy(block(held, b), block(rebuilt_out, b), reb_sem.at[b])
        copy.start()
        rebuilt_copies.append(copy)

    def out_copy(j):
        out, k = (q_out, j) if j < q_blocks else (kv_out, j - q_blocks)
        return pltpu.make_async_copy(outbuf.at[j], out.at[:, pl.ds(k * COLS, COLS)], out_sem.at[j])

    def product(j, start, size):
        part = pl.ds(pl.multiple_of(start, BLK), size)
        return jnp.dot(normed[:, part], wbuf[j, part, :], preferred_element_type=jnp.float32)

    def finish(j, total):
        cols = pl.ds(pl.multiple_of(j * COLS, COLS), COLS)
        outbuf[j] = (total + bias[:, cols]).astype(jnp.bfloat16)

    def near(g):
        for r, cls in ((me, SIB), (ym, D_YM), (yp, D_YP), (xp, D_XP), (y2, D_Y2)):
            arrive(twin(r), g * GRP, GRP, cls, g)
        for r, cls in ((xym, D_XYM), (xyp, D_XYP)):
            arrive(twin(r), g * GRP + 1, 2, cls, g)

    def pair(g):
        near(g)
        arrive(twin(xy2), g * GRP + 1, 2, D_XY2, g)

        def one(j, carry):
            finish(j, product(j, 0, normed.shape[1]))
            return carry

        lax.fori_loop(g * GRP + 1, (g + 1) * GRP, one, 0)
        for j in range(g * GRP + 1, (g + 1) * GRP):
            out_copy(j).start()

    def single(g):
        a = g * GRP
        for r, cls in ((xym, D_XYM_A), (xyp, D_XYP_A), (xy2, D_XY2_A)):
            arrive(twin(r), a, 1, cls, g)

        def one(j, carry):
            finish(j, product(j, 0, normed.shape[1]))
            return carry

        lax.fori_loop(a, a + 1, one, 0)
        out_copy(a).start()

    side = normed.shape[1] // 2
    mine, yours = x * side, (1 - x) * side
    late = (((y + 2) % 4) // 2) * (side // 2)

    def prepare(g):
        near(g)

        def one(k, carry):
            partial[k] = product(g * GRP + 1 + k, mine, side) + product(g * GRP + 1 + k, yours + side // 2 - late, side // 2)
            return carry

        lax.fori_loop(0, GRP - 1, one, 0)

    def complete(g):
        a = g * GRP + 1
        arrive(twin(xy2), a, 2, D_XY2, g)

        def one(k, carry):
            finish(a + k, partial[k] + product(a + k, yours + late, side // 2))
            return carry

        lax.fori_loop(0, GRP - 1, one, 0)
        for j in range(a, a + GRP - 1):
            out_copy(j).start()

    level1(0)
    level1(1)
    relay_first()
    own_x(3)
    beside(0)
    beside(1)
    relay_second()
    own_x(4)
    load_cache.wait()

    @pl.when(sec != 0)
    def _():
        meta_copy().wait_recv()

    level2(0)
    level1(2)
    beside(2)
    opposite_a(0)
    opposite(0)
    own_x(5)
    rebuild(0)
    relay_third()
    level2(1)
    level1(3)
    beside(3)
    opposite_a(1)
    opposite(1)
    far(0)
    rebuild(1)
    level2(2)
    level1(4)
    beside(4)
    opposite_a(2)
    opposite(2)
    far(1)
    rebuild(2)
    rebuild(3)
    pair(0)
    level2(3)
    opposite_a(3)
    opposite(3)
    sides(0)
    pair(1)
    far(2)
    single(0)
    level2(4)
    level1(5)
    beside(5)
    pair(2)
    sides(1)
    opposite_a(4)
    opposite(4)
    single(1)
    far(3)
    sides(2)
    far(4)
    pair(3)
    opposite_a(5)
    single(2)
    pair(4)
    level2(5)
    sides(3)
    sides(4)
    opposite(5)
    single(3)
    single(4)
    sides(5)
    far(5)
    prepare(5)
    single(5)
    complete(5)

    slabs, left = divmod(sum(sent), blocks)
    assert left == 0
    everything = wbuf.at[:, pl.ds(0, slabs * depth), :]
    pltpu.make_async_remote_copy(
        src_ref=everything, dst_ref=everything, send_sem=send, recv_sem=recv.at[0, 0],
        device_id=(sec, other), device_id_type=MESH,
    ).wait_send()
    for copy in rebuilt_copies:
        copy.wait()
    for j in range(blocks):
        out_copy(j).wait()

    @pl.when(sec != last)
    def _():
        meta_copy().wait_send()
        for b in range(row_blocks):
            direct(b).wait_send()

    @pl.when(sec == last)
    def _():
        last_hop(0).wait_send()

    @pl.when(sec == half - 1)
    def _():
        last_hop(1).wait_send()

    @pl.when(sec == half)
    def _():
        last_hop(2).wait_send()

    @pl.when(sec == 0)
    def _():
        over().wait_send()
        across().wait_send()
        last_hop(3).wait_send()


def body(
    cache, payload, block_ids, block_counts, block_scales, refresh_ids, refresh_counts,
    norm_gain, query_weight, query_bias, kv_weight, kv_bias,
):
    rows, feature = cache.shape[1:]
    depth, q_cols = query_weight.shape[1:]
    kv_cols = kv_weight.shape[2]
    blocks = (q_cols + kv_cols) // COLS
    groups = blocks // GRP
    row_blocks = rows // BLK

    anywhere = pl.BlockSpec(memory_space=pl.ANY)
    vmem = pl.BlockSpec(memory_space=pltpu.VMEM)
    dma = pltpu.SemaphoreType.DMA
    rebuilt, queries, keys_values = pl.pallas_call(
        kernel,
        out_shape=(
            jax.ShapeDtypeStruct((rows, feature), jnp.bfloat16),
            jax.ShapeDtypeStruct((rows, q_cols), jnp.bfloat16),
            jax.ShapeDtypeStruct((rows, kv_cols), jnp.bfloat16),
        ),
        in_specs=[anywhere, anywhere, vmem, vmem, vmem, vmem, vmem, vmem, anywhere, vmem, anywhere, vmem],
        out_specs=(anywhere, anywhere, anywhere),
        scratch_shapes=[
            pltpu.VMEM((blocks, feature, COLS), jnp.bfloat16),
            pltpu.VMEM((rows, feature), jnp.bfloat16),
            pltpu.VMEM((rows, feature), jnp.bfloat16),
            pltpu.VMEM((rows, feature), jnp.bfloat16),
            pltpu.VMEM((blocks, rows, COLS), jnp.bfloat16),
            pltpu.VMEM((GRP - 1, rows, COLS), jnp.float32),
            pltpu.VMEM((BLK, feature), jnp.bfloat16),
            pltpu.VMEM((BLK, feature), jnp.bfloat16),
            pltpu.VMEM((BLK, feature), jnp.bfloat16),
            pltpu.VMEM((8, BLK), jnp.int32),
            pltpu.VMEM((8, BLK), jnp.int32),
            pltpu.VMEM((1, q_cols + kv_cols), jnp.float32),
            dma((blocks,)),
            dma,
            dma,
            dma((CLASSES, groups)),
            dma((row_blocks,)),
            dma((row_blocks,)),
            dma,
            dma,
            dma,
            dma,
            dma,
            dma,
            dma,
            dma,
            dma((row_blocks,)),
            dma((blocks,)),
        ],
        compiler_params=pltpu.CompilerParams(collective_id=0, has_side_effects=True, vmem_limit_bytes=64 * 1024 * 1024 - 65536),
        name="boundary",
    )(
        cache[0], payload[0], block_ids[0], block_counts, block_scales[0], refresh_ids[0], refresh_counts,
        norm_gain, query_weight[0], query_bias, kv_weight[0], kv_bias,
    )
    return rebuilt[None], queries[None], keys_values[None]


def solution(mesh):
    in_specs = (
        P("section", "rep", None),
        P("section", "rep", None),
        P("section", "rep", None),
        P("section", "rep"),
        P("section", "rep", None),
        P("section", "rep", None),
        P("section", "rep"),
        P("section", None),
        P("section", "rep", None),
        P("section", None),
        P("section", "rep", None),
        P("section", None),
    )
    out_specs = (P("section", "rep", None), P("section", "rep", None), P("section", "rep", None))
    return jax.shard_map(body, mesh=mesh, in_specs=in_specs, out_specs=out_specs, check_vma=False)
```

```python
import functools

import jax
import jax.numpy as jnp
from jax import lax
from jax.experimental import pallas as pl
from jax.experimental.pallas import tpu as pltpu
from jax.sharding import PartitionSpec as P

EPSILON = 1e-06
BLK = 128
COLS = 256
GRP = 3
MESH = pl.DeviceIdType.MESH

YM, YP, XP = 0, 1, 2
Y2B, Y2C, Y2A = 3, 4, 5
XYM_BC, XYP_BC, XYP_A, XYM_A = 6, 7, 8, 9
XY2B, XY2C, XY2A = 10, 11, 12
D_OWN, D_SIDE, D_FAR, D_A = 13, 14, 15, 16
CLASSES = 17


def kernel(
    cache, payload, ids, counts, scales, refresh_ids, refresh_counts, gain, q_w, q_b, kv_w, kv_b,
    held, outbuf,
    wbuf, pay, normed, partial, relay, relay_two, relay_three, meta, meta_in, bias,
    ld_sem, cache_sem, send, recv, pay_send, pay_recv, meta_send, meta_recv,
    relay_send, relay_recv, two_send, two_recv, three_send, three_recv,
):
    sec = lax.axis_index("section")
    me = lax.axis_index("rep")
    depth = q_w.shape[0]
    q_blocks = q_w.shape[1] // COLS
    blocks = q_blocks + kv_w.shape[1] // COLS
    groups = blocks // GRP
    row_blocks = payload.shape[0] // BLK

    x, y, core = me // 8, (me // 2) % 4, me % 2

    def rank(dx, dy):
        return ((x + dx) % 2) * 8 + ((y + dy) % 4) * 2 + core

    ym, yp, y2 = rank(0, 3), rank(0, 1), rank(0, 2)
    xp, xym, xyp, xy2 = rank(1, 0), rank(1, 3), rank(1, 1), rank(1, 2)
    other = me + 1 - 2 * core

    def region(r, first, count):
        rows = pl.ds(pl.multiple_of(r * depth, 32), depth)
        return wbuf.at[pl.ds(first, count), rows, :]

    def remote(ref, cls, g, to):
        return pltpu.make_async_remote_copy(
            src_ref=ref, dst_ref=ref, send_sem=send, recv_sem=recv.at[cls, g],
            device_id=(sec, to), device_id_type=MESH,
        )

    sent = []

    def push(r, first, count, cls, g, to):
        copy = remote(region(r, first, count), cls, g, to)
        copy.start()
        sent.append(count)

    def arrive(r, first, count, cls, g):
        remote(region(r, first, count), cls, g, other).wait_recv()

    loads = []
    for j in range(blocks):
        if j < q_blocks:
            src = q_w.at[:, pl.ds(j * COLS, COLS)]
        else:
            src = kv_w.at[:, pl.ds((j - q_blocks) * COLS, COLS)]
        rows = pl.ds(pl.multiple_of(me * depth, 32), depth)
        copy = pltpu.make_async_copy(src, wbuf.at[j, rows, :], ld_sem.at[j])
        copy.start()
        loads.append(copy)

    lane = lax.broadcasted_iota(jnp.int32, (1, BLK), 1)

    def two(v):
        return jnp.where(lane == 0, v[:, 0:1], v[:, 1:2])

    meta[0:1, :] = refresh_ids[...]
    meta[1:2, :] = jnp.broadcast_to(refresh_counts[...], (1, BLK))
    meta[2:3, :] = two(ids[...])
    meta[3:4, :] = two(scales[...])
    meta[4:5, :] = jnp.broadcast_to(counts[...], (1, BLK))
    meta[5:8, :] = jnp.zeros((3, BLK), jnp.int32)

    load_cache = pltpu.make_async_copy(cache, held, cache_sem)
    load_cache.start()

    last = lax.axis_size("section") - 1
    half = (last + 1) // 2
    barrier = pltpu.get_barrier_semaphore()

    def greet(to_sec, to_rep):
        pl.semaphore_signal(barrier, inc=1, device_id=(to_sec, to_rep), device_id_type=MESH)

    for r in (ym, yp, xp, other):
        greet(sec, r)
    expected = 4
    pairs = [(s, s + 1, me) for s in range(last)]
    pairs += [(0, half - 1, me), (half - 1, last, xp), (half - 1, half, xp), (half, last, xp), (0, half, xp)]
    for one, two, r in pairs:
        @pl.when(sec == one)
        def _():
            greet(two, r)

        @pl.when(sec == two)
        def _():
            greet(one, r)

        expected = expected + jnp.where((sec == one) | (sec == two), 1, 0)
    pl.semaphore_wait(barrier, expected)

    def block(ref, b):
        return ref.at[pl.ds(b * BLK, BLK), :]

    def pay_copy(src, dst, to_sec, to_rep, send_sem, recv_sem):
        return pltpu.make_async_remote_copy(
            src_ref=src, dst_ref=dst, send_sem=send_sem, recv_sem=recv_sem,
            device_id=(to_sec, to_rep), device_id_type=MESH,
        )

    following = lax.rem(sec + 1, last + 1)

    def direct(b):
        return pay_copy(block(payload, b), block(pay, b), following, me, pay_send.at[b], pay_recv.at[b])

    def first_hop(b):
        to_sec, to_rep = ((last, xp), (half - 1, xp), (0, me), (0, me))[b]
        dst, sem = (relay_two, two_recv) if b == 3 else (relay, relay_recv)
        return pay_copy(block(payload, b), dst, to_sec, to_rep, pay_send.at[b], sem)

    def over():
        return pay_copy(relay, relay, half, xp, relay_send, relay_recv)

    def across():
        return pay_copy(relay_two, relay_three, 0, xp, two_send, three_recv)

    def last_hop(b):
        src, sem = (relay_three, three_send) if b == 3 else (relay, relay_send)
        return pay_copy(src, block(pay, b), half, xp, sem, pay_recv.at[b])

    def relay_first():
        @pl.when(sec == last)
        def _():
            first_hop(0).wait_recv()
            last_hop(0).start()

        @pl.when(sec == 0)
        def _():
            first_hop(2).wait_recv()
            over().start()

    def relay_second():
        @pl.when(sec == half - 1)
        def _():
            first_hop(1).wait_recv()
            last_hop(1).start()

        @pl.when(sec == half)
        def _():
            over().wait_recv()
            last_hop(2).start()

        @pl.when(sec == 0)
        def _():
            first_hop(3).wait_recv()
            across().start()

    def relay_third():
        @pl.when(sec == 0)
        def _():
            across().wait_recv()
            last_hop(3).start()

    def meta_copy():
        return pay_copy(meta, meta_in, following, me, meta_send, meta_recv)

    @pl.when(sec != last)
    def _():
        meta_copy().start()

    @pl.when(sec == half - 1)
    def _():
        for b in (0, 2, 3):
            first_hop(b).start()

    @pl.when((sec != half - 1) & (sec != last))
    def _():
        for b in range(row_blocks):
            direct(b).start()

    def fill(b):
        return pltpu.make_async_copy(block(payload, b), block(pay, b), pay_recv.at[b])

    @pl.when(sec == 0)
    def _():
        meta_in[...] = jnp.zeros((8, BLK), jnp.int32)
        for b in range(row_blocks):
            fill(b).start()

    def own_x(g):
        push(me, g * GRP, GRP, XP, g, xp)

    for g in range(groups):
        for j in range(g * GRP, (g + 1) * GRP):
            loads[j].wait()
        push(me, g * GRP, GRP, YM, g, yp)
        push(me, g * GRP, GRP, YP, g, ym)
        if g < groups // 2:
            own_x(g)
        if g == 1:
            @pl.when(sec == half - 1)
            def _():
                first_hop(1).start()

        push(me, g * GRP, GRP, D_OWN, g, other)

    bias[:, : q_w.shape[1]] = q_b[...]
    bias[:, q_w.shape[1] :] = kv_b[...]

    def level1(g):
        a = g * GRP
        there, source = (yp, ym) if g % 2 == 0 else (ym, yp)
        final = g == groups - 1
        arrive(ym, a, GRP, YM, g)
        arrive(yp, a, GRP, YP, g)
        if final:
            push(source, a, 1, Y2A, g, there)
        arrive(xp, a, GRP, XP, g)
        push(xp, a + 1, 2, XYM_BC, g, yp)
        push(xp, a + 1, 2, XYP_BC, g, ym)
        push(ym, a + 1, 1, Y2B, g, yp)
        push(yp, a + 2, 1, Y2C, g, ym)
        if not final:
            push(source, a, 1, Y2A, g, there)
        push(xp, a, GRP, D_OWN, g, other)
        push(ym, a, GRP, D_OWN, g, other)
        push(yp, a, GRP, D_OWN, g, other)

    def beside(g):
        push(ym, g * GRP, 1, XYM_A, g, xp)
        push(yp, g * GRP, 1, XYP_A, g, xp)

    def level2(g):
        a = g * GRP
        arrive(xym, a + 1, 2, XYM_BC, g)
        push(xym, a + 1, 1, XY2B, g, yp)
        arrive(xyp, a + 1, 2, XYP_BC, g)
        push(xyp, a + 2, 1, XY2C, g, ym)
        push(xym, a + 1, 2, D_SIDE, g, other)
        push(xyp, a + 1, 2, D_SIDE, g, other)

    def opposite_a(g):
        arrive(y2, g * GRP, 1, Y2A, g)
        push(y2, g * GRP, 1, XY2A, g, xp)

    def opposite(g):
        a = g * GRP
        arrive(y2, a + 1, 1, Y2B, g)
        arrive(y2, a + 2, 1, Y2C, g)
        push(y2, a, GRP, D_OWN, g, other)

    def far(g):
        a = g * GRP
        arrive(xy2, a + 1, 1, XY2B, g)
        arrive(xy2, a + 2, 1, XY2C, g)
        push(xy2, a + 1, 2, D_FAR, g, other)

    def sides(g):
        a = g * GRP
        arrive(xym, a, 1, XYM_A, g)
        push(xym, a, 1, D_A, g, other)
        arrive(xyp, a, 1, XYP_A, g)
        push(xyp, a, 1, D_A, g, other)
        arrive(xy2, a, 1, XY2A, g)
        push(xy2, a, 1, D_A, g, other)

    valid = sec > 0

    def rebuild(b):
        @pl.when(sec != 0)
        def _():
            direct(b).wait_recv()

        @pl.when(sec == 0)
        def _():
            fill(b).wait()

        lists = meta_in[...]
        refreshed = jnp.where((lane < lists[1:2, :]) & valid, lists[0:1, :], -1)
        listed = (lane < lists[4:5, :]) & (lane < ids.shape[1]) & (lists[2:3, :] == b) & valid
        factor = jnp.sum(jnp.where(listed, lists[3:4, :].astype(jnp.float32) / 4096.0, 0.0), axis=1, keepdims=True)
        strip = 16

        def one(i, carry):
            start = pl.multiple_of(b * BLK + i * strip, strip)
            rows = pl.ds(start, strip)
            number = lax.broadcasted_iota(jnp.int32, (strip, BLK), 0) + start
            hit = jnp.max(jnp.where(number == refreshed, 1.0, 0.0), axis=1, keepdims=True) > 0.0
            came = pay[rows, :].astype(jnp.float32)
            delta = (came * factor).astype(jnp.bfloat16).astype(jnp.float32)
            mixed = jnp.where(hit, came, held[rows, :].astype(jnp.float32) + delta).astype(jnp.bfloat16)
            held[rows, :] = mixed
            wide = mixed.astype(jnp.float32)
            scale = lax.rsqrt(jnp.mean(wide * wide, axis=1, keepdims=True) + EPSILON)
            normed[rows, :] = (wide * scale * gain[...]).astype(jnp.bfloat16)
            return carry

        lax.fori_loop(0, BLK // strip, one, 0)

    once = jnp.where(me >= 0, 1, 0)

    def product(j, start, size):
        part = pl.ds(pl.multiple_of(start, BLK), size)
        return jnp.dot(normed[:, part], wbuf[j, part, :], preferred_element_type=jnp.float32)

    def finish(j, total):
        cols = pl.ds(pl.multiple_of(j * COLS, COLS), COLS)
        outbuf[j] = (total + bias[:, cols]).astype(jnp.bfloat16)

    def handed(first, count, shards, cls, g):
        whole = wbuf.at[pl.ds(first, count), pl.ds(0, shards * depth), :]
        remote(whole, cls, g, other).wait_recv()

    def near(g):
        handed(g * GRP, GRP, 5, D_OWN, g)
        handed(g * GRP + 1, 2, 2, D_SIDE, g)

    def pair(g):
        near(g)
        handed(g * GRP + 1, 2, 1, D_FAR, g)

        def one(j, carry):
            finish(j, product(j, 0, normed.shape[1]))
            return carry

        lax.fori_loop(g * GRP + 1, (g + 1) * GRP, one, 0)

    def single(g):
        a = g * GRP
        handed(a, 1, 3, D_A, g)

        def one(j, carry):
            finish(j, product(j, 0, normed.shape[1]))
            return carry

        lax.fori_loop(a, a + once, one, 0)

    side = normed.shape[1] // 2
    mine, yours = x * side, (1 - x) * side
    late = (((y + 2) % 4) // 2) * (side // 2)

    def prepare(g):
        near(g)

        def one(k, carry):
            partial[k] = product(g * GRP + 1 + k, mine, side) + product(g * GRP + 1 + k, yours + side // 2 - late, side // 2)
            return carry

        lax.fori_loop(0, GRP - 1, one, 0)

    def complete(g):
        a = g * GRP + 1
        handed(a, 2, 1, D_FAR, g)

        def one(k, carry):
            finish(a + k, partial[k] + product(a + k, yours + late, side // 2))
            return carry

        lax.fori_loop(0, GRP - 1, one, 0)

    level1(0)
    level1(1)
    relay_first()
    own_x(3)
    beside(0)
    beside(1)
    relay_second()
    own_x(4)
    load_cache.wait()

    @pl.when(sec != 0)
    def _():
        meta_copy().wait_recv()

    level2(0)
    level1(2)
    beside(2)
    opposite_a(0)
    opposite(0)
    own_x(5)
    rebuild(0)
    relay_third()
    level2(1)
    level1(3)
    beside(3)
    opposite_a(1)
    opposite(1)
    far(0)
    rebuild(1)
    level2(2)
    level1(4)
    beside(4)
    opposite_a(2)
    opposite(2)
    far(1)
    rebuild(2)
    rebuild(3)
    pair(0)
    level2(3)
    opposite_a(3)
    opposite(3)
    sides(0)
    pair(1)
    far(2)
    single(0)
    pair(2)
    sides(1)
    level2(4)
    level1(5)
    beside(5)
    single(1)
    sides(2)
    opposite_a(4)
    opposite(4)
    single(2)
    far(3)
    sides(3)
    far(4)
    pair(3)
    opposite_a(5)
    single(3)
    pair(4)
    level2(5)
    sides(4)
    opposite(5)
    single(4)
    prepare(5)
    far(5)
    sides(5)
    complete(5)
    single(5)

    slabs, left = divmod(sum(sent), blocks)
    assert left == 0
    everything = wbuf.at[:, pl.ds(0, slabs * depth), :]
    pltpu.make_async_remote_copy(
        src_ref=everything, dst_ref=everything, send_sem=send, recv_sem=recv.at[0, 0],
        device_id=(sec, other), device_id_type=MESH,
    ).wait_send()
    @pl.when(sec != last)
    def _():
        meta_copy().wait_send()
        for b in range(row_blocks):
            direct(b).wait_send()

    @pl.when(sec == last)
    def _():
        last_hop(0).wait_send()

    @pl.when(sec == half - 1)
    def _():
        last_hop(1).wait_send()

    @pl.when(sec == half)
    def _():
        last_hop(2).wait_send()

    @pl.when(sec == 0)
    def _():
        over().wait_send()
        across().wait_send()
        last_hop(3).wait_send()


def write(held, outbuf, rebuilt, queries, keys_values, sem):
    q_blocks = queries.shape[1] // COLS
    copies = [pltpu.make_async_copy(held, rebuilt, sem.at[outbuf.shape[0]])]
    for j in range(outbuf.shape[0]):
        out, k = (queries, j) if j < q_blocks else (keys_values, j - q_blocks)
        copies.append(pltpu.make_async_copy(outbuf.at[j], out.at[:, pl.ds(k * COLS, COLS)], sem.at[j]))
    for copy in copies:
        copy.start()
    for copy in copies:
        copy.wait()


def body(
    cache, payload, block_ids, block_counts, block_scales, refresh_ids, refresh_counts,
    norm_gain, query_weight, query_bias, kv_weight, kv_bias,
):
    rows, feature = cache.shape[1:]
    depth, q_cols = query_weight.shape[1:]
    kv_cols = kv_weight.shape[2]
    blocks = (q_cols + kv_cols) // COLS
    groups = blocks // GRP
    row_blocks = rows // BLK

    anywhere = pl.BlockSpec(memory_space=pl.ANY)
    vmem = pl.BlockSpec(memory_space=pltpu.VMEM)
    dma = pltpu.SemaphoreType.DMA
    held, outbuf = pl.pallas_call(
        kernel,
        out_shape=(
            pltpu.VMEM((rows, feature), jnp.bfloat16),
            pltpu.VMEM((blocks, rows, COLS), jnp.bfloat16),
        ),
        in_specs=[anywhere, anywhere, vmem, vmem, vmem, vmem, vmem, vmem, anywhere, vmem, anywhere, vmem],
        out_specs=(vmem, vmem),
        scratch_shapes=[
            pltpu.VMEM((blocks, feature, COLS), jnp.bfloat16),
            pltpu.VMEM((rows, feature), jnp.bfloat16),
            pltpu.VMEM((rows, feature), jnp.bfloat16),
            pltpu.VMEM((GRP - 1, rows, COLS), jnp.float32),
            pltpu.VMEM((BLK, feature), jnp.bfloat16),
            pltpu.VMEM((BLK, feature), jnp.bfloat16),
            pltpu.VMEM((BLK, feature), jnp.bfloat16),
            pltpu.VMEM((8, BLK), jnp.int32),
            pltpu.VMEM((8, BLK), jnp.int32),
            pltpu.VMEM((1, q_cols + kv_cols), jnp.float32),
            dma((blocks,)),
            dma,
            dma,
            dma((CLASSES, groups)),
            dma((row_blocks,)),
            dma((row_blocks,)),
            dma,
            dma,
            dma,
            dma,
            dma,
            dma,
            dma,
            dma,
        ],
        compiler_params=pltpu.CompilerParams(collective_id=0, has_side_effects=True, vmem_limit_bytes=48 * 1024 * 1024),
        name="boundary",
    )(
        cache[0], payload[0], block_ids[0], block_counts, block_scales[0], refresh_ids[0], refresh_counts,
        norm_gain, query_weight[0], query_bias, kv_weight[0], kv_bias,
    )
    rebuilt, queries, keys_values = pl.pallas_call(
        write,
        out_shape=tuple(jax.ShapeDtypeStruct((rows, n), jnp.bfloat16) for n in (feature, q_cols, kv_cols)),
        in_specs=[vmem, vmem],
        out_specs=(anywhere, anywhere, anywhere),
        scratch_shapes=[dma((blocks + 1,))],
        compiler_params=pltpu.CompilerParams(vmem_limit_bytes=1024 * 1024),
        name="write",
    )(held, outbuf)
    return rebuilt[None], queries[None], keys_values[None]


def solution(mesh):
    in_specs = (
        P("section", "rep", None),
        P("section", "rep", None),
        P("section", "rep", None),
        P("section", "rep"),
        P("section", "rep", None),
        P("section", "rep", None),
        P("section", "rep"),
        P("section", None),
        P("section", "rep", None),
        P("section", None),
        P("section", "rep", None),
        P("section", None),
    )
    out_specs = (P("section", "rep", None), P("section", "rep", None), P("section", "rep", None))
    return jax.shard_map(body, mesh=mesh, in_specs=in_specs, out_specs=out_specs, check_vma=False)
```

```python
import functools

import jax
import jax.numpy as jnp
from jax import lax
from jax.experimental import pallas as pl
from jax.experimental.pallas import tpu as pltpu
from jax.sharding import PartitionSpec as P

EPSILON = 1e-06
BLK = 128
COLS = 256
GRP = 3
MESH = pl.DeviceIdType.MESH

YM, YP, XP = 0, 1, 2
Y2B, Y2C, Y2A = 3, 4, 5
XYM_BC, XYP_BC, XYP_A, XYM_A = 6, 7, 8, 9
XY2B, XY2C, XY2A = 10, 11, 12
D_OWN, D_SIDE, D_FAR, D_A, D_Y2 = 13, 14, 15, 16, 17
CLASSES = 18


def kernel(
    cache, payload, ids, counts, scales, refresh_ids, refresh_counts, gain, q_w, q_b, kv_w, kv_b,
    held, outbuf,
    wbuf, pay, normed, partial, relay, relay_two, relay_three, meta, meta_in, bias,
    ld_sem, cache_sem, send, recv, pay_send, pay_recv, meta_send, meta_recv,
    relay_send, relay_recv, two_send, two_recv, three_send, three_recv,
):
    sec = lax.axis_index("section")
    me = lax.axis_index("rep")
    depth = q_w.shape[0]
    q_blocks = q_w.shape[1] // COLS
    blocks = q_blocks + kv_w.shape[1] // COLS
    groups = blocks // GRP
    row_blocks = payload.shape[0] // BLK

    x, y, core = me // 8, (me // 2) % 4, me % 2

    def rank(dx, dy):
        return ((x + dx) % 2) * 8 + ((y + dy) % 4) * 2 + core

    ym, yp, y2 = rank(0, 3), rank(0, 1), rank(0, 2)
    xp, xym, xyp, xy2 = rank(1, 0), rank(1, 3), rank(1, 1), rank(1, 2)
    other = me + 1 - 2 * core

    def region(r, first, count):
        rows = pl.ds(pl.multiple_of(r * depth, 32), depth)
        return wbuf.at[pl.ds(first, count), rows, :]

    def remote(ref, cls, g, to):
        return pltpu.make_async_remote_copy(
            src_ref=ref, dst_ref=ref, send_sem=send, recv_sem=recv.at[cls, g],
            device_id=(sec, to), device_id_type=MESH,
        )

    sent = []

    def push(r, first, count, cls, g, to):
        copy = remote(region(r, first, count), cls, g, to)
        copy.start()
        sent.append(count)

    def arrive(r, first, count, cls, g):
        remote(region(r, first, count), cls, g, other).wait_recv()

    loads = []
    for j in range(blocks):
        if j < q_blocks:
            src = q_w.at[:, pl.ds(j * COLS, COLS)]
        else:
            src = kv_w.at[:, pl.ds((j - q_blocks) * COLS, COLS)]
        rows = pl.ds(pl.multiple_of(me * depth, 32), depth)
        copy = pltpu.make_async_copy(src, wbuf.at[j, rows, :], ld_sem.at[j])
        copy.start()
        loads.append(copy)

    lane = lax.broadcasted_iota(jnp.int32, (1, BLK), 1)

    def two(v):
        return jnp.where(lane == 0, v[:, 0:1], v[:, 1:2])

    meta[0:1, :] = refresh_ids[...]
    meta[1:2, :] = jnp.broadcast_to(refresh_counts[...], (1, BLK))
    meta[2:3, :] = two(ids[...])
    meta[3:4, :] = two(scales[...])
    meta[4:5, :] = jnp.broadcast_to(counts[...], (1, BLK))
    meta[5:8, :] = jnp.zeros((3, BLK), jnp.int32)

    load_cache = pltpu.make_async_copy(cache, held, cache_sem)
    load_cache.start()

    last = lax.axis_size("section") - 1
    half = (last + 1) // 2
    barrier = pltpu.get_barrier_semaphore()

    def greet(to_sec, to_rep):
        pl.semaphore_signal(barrier, inc=1, device_id=(to_sec, to_rep), device_id_type=MESH)

    for r in (ym, yp, xp, other):
        greet(sec, r)
    expected = 4
    links = [(s + 1, s, me) for s in range(last)]
    links += [(0, half - 1, me), (last, half - 1, xp), (half, half - 1, xp), (half, last, xp), (half, 0, xp)]
    for receiver, sender, r in links:
        @pl.when(sec == receiver)
        def _():
            greet(sender, r)

        expected = expected + jnp.where(sec == sender, 1, 0)
    pl.semaphore_wait(barrier, expected)

    def block(ref, b):
        return ref.at[pl.ds(b * BLK, BLK), :]

    def pay_copy(src, dst, to_sec, to_rep, send_sem, recv_sem):
        return pltpu.make_async_remote_copy(
            src_ref=src, dst_ref=dst, send_sem=send_sem, recv_sem=recv_sem,
            device_id=(to_sec, to_rep), device_id_type=MESH,
        )

    following = lax.rem(sec + 1, last + 1)

    def direct(b):
        return pay_copy(block(payload, b), block(pay, b), following, me, pay_send.at[b], pay_recv.at[b])

    def first_hop(b):
        to_sec, to_rep = ((last, xp), (half - 1, xp), (0, me), (0, me))[b]
        dst, sem = (relay_two, two_recv) if b == 3 else (relay, relay_recv)
        return pay_copy(block(payload, b), dst, to_sec, to_rep, pay_send.at[b], sem)

    def over():
        return pay_copy(relay, relay, half, xp, relay_send, relay_recv)

    def across():
        return pay_copy(relay_two, relay_three, 0, xp, two_send, three_recv)

    def last_hop(b):
        src, sem = (relay_three, three_send) if b == 3 else (relay, relay_send)
        return pay_copy(src, block(pay, b), half, xp, sem, pay_recv.at[b])

    def relay_first():
        @pl.when(sec == last)
        def _():
            first_hop(0).wait_recv()
            last_hop(0).start()

        @pl.when(sec == 0)
        def _():
            first_hop(2).wait_recv()
            over().start()

    def relay_second():
        @pl.when(sec == half - 1)
        def _():
            first_hop(1).wait_recv()
            last_hop(1).start()

        @pl.when(sec == half)
        def _():
            over().wait_recv()
            last_hop(2).start()

        @pl.when(sec == 0)
        def _():
            first_hop(3).wait_recv()
            across().start()

    def relay_third():
        @pl.when(sec == 0)
        def _():
            across().wait_recv()
            last_hop(3).start()

    def meta_copy():
        return pay_copy(meta, meta_in, following, me, meta_send, meta_recv)

    @pl.when(sec != last)
    def _():
        meta_copy().start()

    @pl.when(sec == half - 1)
    def _():
        for b in (0, 2, 3):
            first_hop(b).start()

    @pl.when((sec != half - 1) & (sec != last))
    def _():
        for b in range(row_blocks):
            direct(b).start()

    def fill(b):
        return pltpu.make_async_copy(block(payload, b), block(pay, b), pay_recv.at[b])

    @pl.when(sec == 0)
    def _():
        meta_in[...] = jnp.zeros((8, BLK), jnp.int32)
        for b in range(row_blocks):
            fill(b).start()

    def own_x(g):
        push(me, g * GRP, GRP, XP, g, xp)

    for g in range(groups):
        for j in range(g * GRP, (g + 1) * GRP):
            loads[j].wait()
        push(me, g * GRP, GRP, YM, g, yp)
        push(me, g * GRP, GRP, YP, g, ym)
        if g < groups // 2:
            own_x(g)
        if g == 1:
            @pl.when(sec == half - 1)
            def _():
                first_hop(1).start()

        push(me, g * GRP, GRP, D_OWN, g, other)

    bias[:, : q_w.shape[1]] = q_b[...]
    bias[:, q_w.shape[1] :] = kv_b[...]

    def level1(g):
        a = g * GRP
        there, source = (yp, ym) if g % 2 == 0 else (ym, yp)
        final = g == groups - 1
        arrive(ym, a, GRP, YM, g)
        arrive(yp, a, GRP, YP, g)
        if final:
            push(source, a, 1, Y2A, g, there)
        arrive(xp, a, GRP, XP, g)
        push(xp, a + 1, 2, XYM_BC, g, yp)
        push(xp, a + 1, 2, XYP_BC, g, ym)
        push(ym, a + 1, 1, Y2B, g, yp)
        push(yp, a + 2, 1, Y2C, g, ym)
        if not final:
            push(source, a, 1, Y2A, g, there)
        push(xp, a, GRP, D_OWN, g, other)
        push(ym, a, GRP, D_OWN, g, other)
        push(yp, a, GRP, D_OWN, g, other)

    def beside(g):
        push(ym, g * GRP, 1, XYM_A, g, xp)
        push(yp, g * GRP, 1, XYP_A, g, xp)

    def level2_up(g):
        arrive(xym, g * GRP + 1, 2, XYM_BC, g)
        push(xym, g * GRP + 1, 1, XY2B, g, yp)
        push(xym, g * GRP + 1, 2, D_SIDE, g, other)

    def level2_down(g):
        arrive(xyp, g * GRP + 1, 2, XYP_BC, g)
        push(xyp, g * GRP + 2, 1, XY2C, g, ym)
        push(xyp, g * GRP + 1, 2, D_SIDE, g, other)

    def level2(g):
        level2_up(g)
        level2_down(g)

    def opposite_a(g):
        arrive(y2, g * GRP, 1, Y2A, g)
        push(y2, g * GRP, 1, XY2A, g, xp)

    def opposite(g):
        a = g * GRP
        arrive(y2, a + 1, 1, Y2B, g)
        arrive(y2, a + 2, 1, Y2C, g)
        push(y2, a, GRP, D_Y2, g, other)

    def far(g):
        a = g * GRP
        arrive(xy2, a + 1, 1, XY2B, g)
        arrive(xy2, a + 2, 1, XY2C, g)
        push(xy2, a + 1, 2, D_FAR, g, other)

    def sides(g):
        a = g * GRP
        arrive(xym, a, 1, XYM_A, g)
        push(xym, a, 1, D_A, g, other)
        arrive(xyp, a, 1, XYP_A, g)
        push(xyp, a, 1, D_A, g, other)
        arrive(xy2, a, 1, XY2A, g)
        push(xy2, a, 1, D_A, g, other)

    valid = sec > 0

    def rebuild(b):
        @pl.when(sec != 0)
        def _():
            direct(b).wait_recv()

        @pl.when(sec == 0)
        def _():
            fill(b).wait()

        lists = meta_in[...]
        refreshed = jnp.where((lane < lists[1:2, :]) & valid, lists[0:1, :], -1)
        listed = (lane < lists[4:5, :]) & (lane < ids.shape[1]) & (lists[2:3, :] == b) & valid
        factor = jnp.sum(jnp.where(listed, lists[3:4, :].astype(jnp.float32) / 4096.0, 0.0), axis=1, keepdims=True)
        strip = 16

        def one(i, carry):
            start = pl.multiple_of(b * BLK + i * strip, strip)
            rows = pl.ds(start, strip)
            number = lax.broadcasted_iota(jnp.int32, (strip, BLK), 0) + start
            hit = jnp.max(jnp.where(number == refreshed, 1.0, 0.0), axis=1, keepdims=True) > 0.0
            came = pay[rows, :].astype(jnp.float32)
            delta = (came * factor).astype(jnp.bfloat16).astype(jnp.float32)
            mixed = jnp.where(hit, came, held[rows, :].astype(jnp.float32) + delta).astype(jnp.bfloat16)
            held[rows, :] = mixed
            wide = mixed.astype(jnp.float32)
            scale = lax.rsqrt(jnp.mean(wide * wide, axis=1, keepdims=True) + EPSILON)
            normed[rows, :] = (wide * scale * gain[...]).astype(jnp.bfloat16)
            return carry

        lax.fori_loop(0, BLK // strip, one, 0)

    once = jnp.where(me >= 0, 1, 0)

    def product(j, start, size):
        part = pl.ds(pl.multiple_of(start, BLK), size)
        return jnp.dot(normed[:, part], wbuf[j, part, :], preferred_element_type=jnp.float32)

    def finish(j, total):
        cols = pl.ds(pl.multiple_of(j * COLS, COLS), COLS)
        outbuf[j] = (total + bias[:, cols]).astype(jnp.bfloat16)

    def handed(first, count, shards, cls, g):
        whole = wbuf.at[pl.ds(first, count), pl.ds(0, shards * depth), :]
        remote(whole, cls, g, other).wait_recv()

    def near(g):
        handed(g * GRP, GRP, 4, D_OWN, g)
        handed(g * GRP + 1, 2, 2, D_SIDE, g)

    def pair(g):
        near(g)
        handed(g * GRP, GRP, 1, D_Y2, g)
        handed(g * GRP + 1, 2, 1, D_FAR, g)

        def one(j, carry):
            finish(j, product(j, 0, normed.shape[1]))
            return carry

        lax.fori_loop(g * GRP + 1, (g + 1) * GRP, one, 0)

    def single(g):
        a = g * GRP
        handed(a, 1, 3, D_A, g)

        def one(j, carry):
            finish(j, product(j, 0, normed.shape[1]))
            return carry

        lax.fori_loop(a, a + once, one, 0)

    side = normed.shape[1] // 2
    quarter = side // 2
    mine, yours = x * side, (1 - x) * side
    late = (((y + 2) % 4) // 2) * quarter
    soon = quarter - late

    def prepare(g):
        a = g * GRP + 1
        near(g)

        def one(k, carry):
            partial[k] = product(a + k, mine + soon, quarter) + product(a + k, yours + soon, quarter)
            return carry

        lax.fori_loop(0, GRP - 1, one, 0)

    def extend(g):
        a = g * GRP + 1
        handed(g * GRP, GRP, 1, D_Y2, g)

        def one(k, carry):
            partial[k] += product(a + k, mine + late, quarter)
            return carry

        lax.fori_loop(0, GRP - 1, one, 0)

    def complete(g):
        a = g * GRP + 1
        handed(a, 2, 1, D_FAR, g)

        def one(k, carry):
            finish(a + k, partial[k] + product(a + k, yours + late, quarter))
            return carry

        lax.fori_loop(0, GRP - 1, one, 0)

    level1(0)
    level1(1)
    relay_first()
    own_x(3)
    beside(0)
    beside(1)
    relay_second()
    own_x(4)
    load_cache.wait()

    @pl.when(sec != 0)
    def _():
        meta_copy().wait_recv()

    level2(0)
    level1(2)
    beside(2)
    opposite_a(0)
    opposite(0)
    own_x(5)
    rebuild(0)
    relay_third()
    level2(1)
    level1(3)
    beside(3)
    opposite_a(1)
    opposite(1)
    far(0)
    rebuild(1)
    level2(2)
    level1(4)
    beside(4)
    opposite_a(2)
    opposite(2)
    far(1)
    rebuild(2)
    rebuild(3)
    pair(0)
    level2(3)
    opposite_a(3)
    opposite(3)
    sides(0)
    pair(1)
    far(2)
    single(0)
    pair(2)
    sides(1)
    level2(4)
    level1(5)
    beside(5)
    single(1)
    opposite_a(4)
    opposite(4)
    far(3)
    far(4)
    sides(2)
    pair(3)
    opposite_a(5)
    sides(3)
    single(2)
    pair(4)
    level2_up(5)
    level2_down(5)
    opposite(5)
    single(3)
    prepare(5)
    far(5)
    sides(4)
    sides(5)
    extend(5)
    complete(5)
    single(4)
    single(5)

    slabs, left = divmod(sum(sent), blocks)
    assert left == 0
    everything = wbuf.at[:, pl.ds(0, slabs * depth), :]
    pltpu.make_async_remote_copy(
        src_ref=everything, dst_ref=everything, send_sem=send, recv_sem=recv.at[0, 0],
        device_id=(sec, other), device_id_type=MESH,
    ).wait_send()
    @pl.when(sec != last)
    def _():
        meta_copy().wait_send()
        for b in range(row_blocks):
            direct(b).wait_send()

    @pl.when(sec == last)
    def _():
        last_hop(0).wait_send()

    @pl.when(sec == half - 1)
    def _():
        last_hop(1).wait_send()

    @pl.when(sec == half)
    def _():
        last_hop(2).wait_send()

    @pl.when(sec == 0)
    def _():
        over().wait_send()
        across().wait_send()
        last_hop(3).wait_send()


def write(held, outbuf, rebuilt, queries, keys_values, sem):
    q_blocks = queries.shape[1] // COLS
    copies = [pltpu.make_async_copy(held, rebuilt, sem.at[outbuf.shape[0]])]
    for j in range(outbuf.shape[0]):
        out, k = (queries, j) if j < q_blocks else (keys_values, j - q_blocks)
        copies.append(pltpu.make_async_copy(outbuf.at[j], out.at[:, pl.ds(k * COLS, COLS)], sem.at[j]))
    for copy in copies:
        copy.start()
    for copy in copies:
        copy.wait()


def body(
    cache, payload, block_ids, block_counts, block_scales, refresh_ids, refresh_counts,
    norm_gain, query_weight, query_bias, kv_weight, kv_bias,
):
    rows, feature = cache.shape[1:]
    depth, q_cols = query_weight.shape[1:]
    kv_cols = kv_weight.shape[2]
    blocks = (q_cols + kv_cols) // COLS
    groups = blocks // GRP
    row_blocks = rows // BLK

    anywhere = pl.BlockSpec(memory_space=pl.ANY)
    vmem = pl.BlockSpec(memory_space=pltpu.VMEM)
    dma = pltpu.SemaphoreType.DMA
    held, outbuf = pl.pallas_call(
        kernel,
        out_shape=(
            pltpu.VMEM((rows, feature), jnp.bfloat16),
            pltpu.VMEM((blocks, rows, COLS), jnp.bfloat16),
        ),
        in_specs=[anywhere, anywhere, vmem, vmem, vmem, vmem, vmem, vmem, anywhere, vmem, anywhere, vmem],
        out_specs=(vmem, vmem),
        scratch_shapes=[
            pltpu.VMEM((blocks, feature, COLS), jnp.bfloat16),
            pltpu.VMEM((rows, feature), jnp.bfloat16),
            pltpu.VMEM((rows, feature), jnp.bfloat16),
            pltpu.VMEM((GRP - 1, rows, COLS), jnp.float32),
            pltpu.VMEM((BLK, feature), jnp.bfloat16),
            pltpu.VMEM((BLK, feature), jnp.bfloat16),
            pltpu.VMEM((BLK, feature), jnp.bfloat16),
            pltpu.VMEM((8, BLK), jnp.int32),
            pltpu.VMEM((8, BLK), jnp.int32),
            pltpu.VMEM((1, q_cols + kv_cols), jnp.float32),
            dma((blocks,)),
            dma,
            dma,
            dma((CLASSES, groups)),
            dma((row_blocks,)),
            dma((row_blocks,)),
            dma,
            dma,
            dma,
            dma,
            dma,
            dma,
            dma,
            dma,
        ],
        compiler_params=pltpu.CompilerParams(collective_id=0, has_side_effects=True, vmem_limit_bytes=48 * 1024 * 1024),
        name="boundary",
    )(
        cache[0], payload[0], block_ids[0], block_counts, block_scales[0], refresh_ids[0], refresh_counts,
        norm_gain, query_weight[0], query_bias, kv_weight[0], kv_bias,
    )
    rebuilt, queries, keys_values = pl.pallas_call(
        write,
        out_shape=tuple(jax.ShapeDtypeStruct((rows, n), jnp.bfloat16) for n in (feature, q_cols, kv_cols)),
        in_specs=[vmem, vmem],
        out_specs=(anywhere, anywhere, anywhere),
        scratch_shapes=[dma((blocks + 1,))],
        compiler_params=pltpu.CompilerParams(vmem_limit_bytes=1024 * 1024),
        name="write",
    )(held, outbuf)
    return rebuilt[None], queries[None], keys_values[None]


def solution(mesh):
    in_specs = (
        P("section", "rep", None),
        P("section", "rep", None),
        P("section", "rep", None),
        P("section", "rep"),
        P("section", "rep", None),
        P("section", "rep", None),
        P("section", "rep"),
        P("section", None),
        P("section", "rep", None),
        P("section", None),
        P("section", "rep", None),
        P("section", None),
    )
    out_specs = (P("section", "rep", None), P("section", "rep", None), P("section", "rep", None))
    return jax.shard_map(body, mesh=mesh, in_specs=in_specs, out_specs=out_specs, check_vma=False)
```

```python
import functools

import jax
import jax.numpy as jnp
from jax import lax
from jax.experimental import pallas as pl
from jax.experimental.pallas import tpu as pltpu
from jax.sharding import PartitionSpec as P

EPSILON = 1e-06
BLK = 128
COLS = 256
GRP = 3
MESH = pl.DeviceIdType.MESH

YM, YP, XP = 0, 1, 2
Y2B, Y2C, Y2A = 3, 4, 5
XYM_BC, XYP_BC, XYP_A, XYM_A = 6, 7, 8, 9
XY2B, XY2C, XY2A = 10, 11, 12
D_OWN, D_SIDE, D_FAR, D_A, D_Y2 = 13, 14, 15, 16, 17
CLASSES = 18


def quarters(x, y, extent):
    side = extent // 2
    return side, side // 2, (((y + 2) % 4) // 2) * (side // 2)


def kernel(
    cache, payload, ids, counts, scales, refresh_ids, refresh_counts, gain, q_w, q_b, kv_w, kv_b,
    held, outbuf, wlast, normed, partial,
    wbuf, pay, relay, relay_two, relay_three, meta, meta_in, bias,
    ld_sem, cache_sem, send, recv, pay_send, pay_recv, meta_send, meta_recv,
    relay_send, relay_recv, two_send, two_recv, three_send, three_recv,
):
    sec = lax.axis_index("section")
    me = lax.axis_index("rep")
    depth = q_w.shape[0]
    q_blocks = q_w.shape[1] // COLS
    blocks = q_blocks + kv_w.shape[1] // COLS
    groups = blocks // GRP
    row_blocks = payload.shape[0] // BLK

    x, y, core = me // 8, (me // 2) % 4, me % 2

    def rank(dx, dy):
        return ((x + dx) % 2) * 8 + ((y + dy) % 4) * 2 + core

    ym, yp, y2 = rank(0, 3), rank(0, 1), rank(0, 2)
    xp, xym, xyp, xy2 = rank(1, 0), rank(1, 3), rank(1, 1), rank(1, 2)
    other = me + 1 - 2 * core

    split = blocks - GRP

    def part(first, count, start, size):
        buf, first = (wbuf, first) if first < split else (wlast, first - split)
        return buf.at[pl.ds(first, count), pl.ds(start, size), :]

    def region(r, first, count):
        return part(first, count, pl.multiple_of(r * depth, 32), depth)

    def remote(ref, cls, g, to):
        return pltpu.make_async_remote_copy(
            src_ref=ref, dst_ref=ref, send_sem=send.at[g // (groups - 1)], recv_sem=recv.at[cls, g],
            device_id=(sec, to), device_id_type=MESH,
        )

    sent = [0, 0]

    def push(r, first, count, cls, g, to):
        copy = remote(region(r, first, count), cls, g, to)
        copy.start()
        sent[g // (groups - 1)] += count

    def arrive(r, first, count, cls, g):
        remote(region(r, first, count), cls, g, other).wait_recv()

    loads = []
    for j in range(blocks):
        if j < q_blocks:
            src = q_w.at[:, pl.ds(j * COLS, COLS)]
        else:
            src = kv_w.at[:, pl.ds((j - q_blocks) * COLS, COLS)]
        buf, k = (wbuf, j) if j < split else (wlast, j - split)
        rows = pl.ds(pl.multiple_of(me * depth, 32), depth)
        copy = pltpu.make_async_copy(src, buf.at[k, rows, :], ld_sem.at[j])
        copy.start()
        loads.append(copy)

    lane = lax.broadcasted_iota(jnp.int32, (1, BLK), 1)

    def two(v):
        return jnp.where(lane == 0, v[:, 0:1], v[:, 1:2])

    meta[0:1, :] = refresh_ids[...]
    meta[1:2, :] = jnp.broadcast_to(refresh_counts[...], (1, BLK))
    meta[2:3, :] = two(ids[...])
    meta[3:4, :] = two(scales[...])
    meta[4:5, :] = jnp.broadcast_to(counts[...], (1, BLK))
    meta[5:8, :] = jnp.zeros((3, BLK), jnp.int32)

    load_cache = pltpu.make_async_copy(cache, held, cache_sem)
    load_cache.start()

    last = lax.axis_size("section") - 1
    half = (last + 1) // 2
    barrier = pltpu.get_barrier_semaphore()

    def greet(to_sec, to_rep):
        pl.semaphore_signal(barrier, inc=1, device_id=(to_sec, to_rep), device_id_type=MESH)

    for r in (ym, yp, xp, other):
        greet(sec, r)
    expected = 4
    links = [(s + 1, s, me) for s in range(last)]
    links += [(0, half - 1, me), (last, half - 1, xp), (half, half - 1, xp), (half, last, xp), (half, 0, xp)]
    for receiver, sender, r in links:
        @pl.when(sec == receiver)
        def _():
            greet(sender, r)

        expected = expected + jnp.where(sec == sender, 1, 0)
    pl.semaphore_wait(barrier, expected)

    def block(ref, b):
        return ref.at[pl.ds(b * BLK, BLK), :]

    def pay_copy(src, dst, to_sec, to_rep, send_sem, recv_sem):
        return pltpu.make_async_remote_copy(
            src_ref=src, dst_ref=dst, send_sem=send_sem, recv_sem=recv_sem,
            device_id=(to_sec, to_rep), device_id_type=MESH,
        )

    following = lax.rem(sec + 1, last + 1)

    def direct(b):
        return pay_copy(block(payload, b), block(pay, b), following, me, pay_send.at[b], pay_recv.at[b])

    def first_hop(b):
        to_sec, to_rep = ((last, xp), (half - 1, xp), (0, me), (0, me))[b]
        dst, sem = (relay_two, two_recv) if b == 3 else (relay, relay_recv)
        return pay_copy(block(payload, b), dst, to_sec, to_rep, pay_send.at[b], sem)

    def over():
        return pay_copy(relay, relay, half, xp, relay_send, relay_recv)

    def across():
        return pay_copy(relay_two, relay_three, 0, xp, two_send, three_recv)

    def last_hop(b):
        src, sem = (relay_three, three_send) if b == 3 else (relay, relay_send)
        return pay_copy(src, block(pay, b), half, xp, sem, pay_recv.at[b])

    def relay_first():
        @pl.when(sec == last)
        def _():
            first_hop(0).wait_recv()
            last_hop(0).start()

        @pl.when(sec == 0)
        def _():
            first_hop(2).wait_recv()
            over().start()

    def relay_second():
        @pl.when(sec == half - 1)
        def _():
            first_hop(1).wait_recv()
            last_hop(1).start()

        @pl.when(sec == half)
        def _():
            over().wait_recv()
            last_hop(2).start()

        @pl.when(sec == 0)
        def _():
            first_hop(3).wait_recv()
            across().start()

    def relay_third():
        @pl.when(sec == 0)
        def _():
            across().wait_recv()
            last_hop(3).start()

    def meta_copy():
        return pay_copy(meta, meta_in, following, me, meta_send, meta_recv)

    @pl.when(sec != last)
    def _():
        meta_copy().start()

    @pl.when(sec == half - 1)
    def _():
        for b in (0, 2, 3):
            first_hop(b).start()

    @pl.when((sec != half - 1) & (sec != last))
    def _():
        for b in range(row_blocks):
            direct(b).start()

    def fill(b):
        return pltpu.make_async_copy(block(payload, b), block(pay, b), pay_recv.at[b])

    @pl.when(sec == 0)
    def _():
        meta_in[...] = jnp.zeros((8, BLK), jnp.int32)
        for b in range(row_blocks):
            fill(b).start()

    def own_x(g):
        push(me, g * GRP, GRP, XP, g, xp)

    for g in range(groups):
        for j in range(g * GRP, (g + 1) * GRP):
            loads[j].wait()
        push(me, g * GRP, GRP, YM, g, yp)
        push(me, g * GRP, GRP, YP, g, ym)
        if g < groups // 2:
            own_x(g)
        if g == 1:
            @pl.when(sec == half - 1)
            def _():
                first_hop(1).start()

        push(me, g * GRP, GRP, D_OWN, g, other)

    bias[:, : q_w.shape[1]] = q_b[...]
    bias[:, q_w.shape[1] :] = kv_b[...]

    def level1(g):
        a = g * GRP
        there, source = (yp, ym) if g % 2 == 0 else (ym, yp)
        final = g == groups - 1
        arrive(ym, a, GRP, YM, g)
        arrive(yp, a, GRP, YP, g)
        if final:
            push(source, a, 1, Y2A, g, there)
        arrive(xp, a, GRP, XP, g)
        push(xp, a + 1, 2, XYM_BC, g, yp)
        push(xp, a + 1, 2, XYP_BC, g, ym)
        push(ym, a + 1, 1, Y2B, g, yp)
        push(yp, a + 2, 1, Y2C, g, ym)
        if not final:
            push(source, a, 1, Y2A, g, there)
        push(xp, a, GRP, D_OWN, g, other)
        push(ym, a, GRP, D_OWN, g, other)
        push(yp, a, GRP, D_OWN, g, other)

    def beside(g):
        push(ym, g * GRP, 1, XYM_A, g, xp)
        push(yp, g * GRP, 1, XYP_A, g, xp)

    def level2_up(g):
        arrive(xym, g * GRP + 1, 2, XYM_BC, g)
        push(xym, g * GRP + 1, 1, XY2B, g, yp)
        push(xym, g * GRP + 1, 2, D_SIDE, g, other)

    def level2_down(g):
        arrive(xyp, g * GRP + 1, 2, XYP_BC, g)
        push(xyp, g * GRP + 2, 1, XY2C, g, ym)
        push(xyp, g * GRP + 1, 2, D_SIDE, g, other)

    def level2(g):
        level2_up(g)
        level2_down(g)

    def opposite_a(g):
        arrive(y2, g * GRP, 1, Y2A, g)
        push(y2, g * GRP, 1, XY2A, g, xp)

    def opposite(g):
        a = g * GRP
        arrive(y2, a + 1, 1, Y2B, g)
        arrive(y2, a + 2, 1, Y2C, g)
        push(y2, a, GRP, D_Y2, g, other)

    def far(g):
        a = g * GRP
        arrive(xy2, a + 1, 1, XY2B, g)
        arrive(xy2, a + 2, 1, XY2C, g)
        push(xy2, a + 1, 2, D_FAR, g, other)

    def sides(g):
        a = g * GRP
        arrive(xym, a, 1, XYM_A, g)
        push(xym, a, 1, D_A, g, other)
        arrive(xyp, a, 1, XYP_A, g)
        push(xyp, a, 1, D_A, g, other)
        arrive(xy2, a, 1, XY2A, g)
        push(xy2, a, 1, D_A, g, other)

    valid = sec > 0

    def rebuild(b):
        @pl.when(sec != 0)
        def _():
            direct(b).wait_recv()

        @pl.when(sec == 0)
        def _():
            fill(b).wait()

        lists = meta_in[...]
        refreshed = jnp.where((lane < lists[1:2, :]) & valid, lists[0:1, :], -1)
        listed = (lane < lists[4:5, :]) & (lane < ids.shape[1]) & (lists[2:3, :] == b) & valid
        factor = jnp.sum(jnp.where(listed, lists[3:4, :].astype(jnp.float32) / 4096.0, 0.0), axis=1, keepdims=True)
        strip = 16

        def one(i, carry):
            start = pl.multiple_of(b * BLK + i * strip, strip)
            rows = pl.ds(start, strip)
            number = lax.broadcasted_iota(jnp.int32, (strip, BLK), 0) + start
            hit = jnp.max(jnp.where(number == refreshed, 1.0, 0.0), axis=1, keepdims=True) > 0.0
            came = pay[rows, :].astype(jnp.float32)
            delta = (came * factor).astype(jnp.bfloat16).astype(jnp.float32)
            mixed = jnp.where(hit, came, held[rows, :].astype(jnp.float32) + delta).astype(jnp.bfloat16)
            held[rows, :] = mixed
            wide = mixed.astype(jnp.float32)
            scale = lax.rsqrt(jnp.mean(wide * wide, axis=1, keepdims=True) + EPSILON)
            normed[rows, :] = (wide * scale * gain[...]).astype(jnp.bfloat16)
            return carry

        lax.fori_loop(0, BLK // strip, one, 0)

    once = jnp.where(me >= 0, 1, 0)

    def product(buf, j, start, size):
        cut = pl.ds(pl.multiple_of(start, BLK), size)
        return jnp.dot(normed[:, cut], buf[j, cut, :], preferred_element_type=jnp.float32)

    def finish(j, total):
        cols = pl.ds(pl.multiple_of(j * COLS, COLS), COLS)
        outbuf[j] = (total + bias[:, cols]).astype(jnp.bfloat16)

    def handed(first, count, shards, cls, g):
        remote(part(first, count, 0, shards * depth), cls, g, other).wait_recv()

    def near(g):
        handed(g * GRP, GRP, 4, D_OWN, g)
        handed(g * GRP + 1, 2, 2, D_SIDE, g)

    def pair(g):
        near(g)
        handed(g * GRP, GRP, 1, D_Y2, g)
        handed(g * GRP + 1, 2, 1, D_FAR, g)

        def one(j, carry):
            finish(j, product(wbuf, j, 0, normed.shape[1]))
            return carry

        lax.fori_loop(g * GRP + 1, (g + 1) * GRP, one, 0)

    def single(g):
        a = g * GRP
        handed(a, 1, 3, D_A, g)

        def one(j, carry):
            finish(j, product(wbuf, j, 0, normed.shape[1]))
            return carry

        lax.fori_loop(a, a + once, one, 0)

    side, quarter, late = quarters(x, y, normed.shape[1])
    mine, yours, soon = x * side, (1 - x) * side, quarter - late

    def prepare(g):
        near(g)

        def one(k, carry):
            partial[k] = product(wlast, 1 + k, mine + soon, quarter) + product(wlast, 1 + k, yours + soon, quarter)
            return carry

        lax.fori_loop(0, GRP - 1, one, 0)

    def extend(g):
        handed(g * GRP, GRP, 1, D_Y2, g)

        def one(k, carry):
            partial[k] += product(wlast, 1 + k, mine + late, quarter)
            return carry

        lax.fori_loop(0, GRP - 1, one, 0)

    level1(0)
    level1(1)
    relay_first()
    own_x(3)
    beside(0)
    beside(1)
    relay_second()
    own_x(4)
    load_cache.wait()

    @pl.when(sec != 0)
    def _():
        meta_copy().wait_recv()

    level2(0)
    level1(2)
    beside(2)
    opposite_a(0)
    opposite(0)
    own_x(5)
    rebuild(0)
    relay_third()
    level2(1)
    level1(3)
    beside(3)
    opposite_a(1)
    opposite(1)
    far(0)
    rebuild(1)
    level2(2)
    level1(4)
    beside(4)
    opposite_a(2)
    opposite(2)
    far(1)
    rebuild(2)
    rebuild(3)
    pair(0)
    level2(3)
    opposite_a(3)
    opposite(3)
    sides(0)
    pair(1)
    far(2)
    single(0)
    pair(2)
    sides(1)
    level2(4)
    level1(5)
    beside(5)
    single(1)
    opposite_a(4)
    opposite(4)
    far(3)
    far(4)
    sides(2)
    pair(3)
    opposite_a(5)
    sides(3)
    single(2)
    pair(4)
    level2_up(5)
    level2_down(5)
    opposite(5)
    single(3)
    prepare(5)
    far(5)
    sides(4)
    sides(5)
    extend(5)
    single(4)
    handed(5 * GRP + 1, 2, 1, D_FAR, 5)
    handed(5 * GRP, 1, 3, D_A, 5)

    for k, buf in enumerate((wbuf, wlast)):
        slabs, left = divmod(sent[k], buf.shape[0])
        assert left == 0
        everything = buf.at[:, pl.ds(0, slabs * depth), :]
        pltpu.make_async_remote_copy(
            src_ref=everything, dst_ref=everything, send_sem=send.at[k], recv_sem=recv.at[0, 0],
            device_id=(sec, other), device_id_type=MESH,
        ).wait_send()

    @pl.when(sec != last)
    def _():
        meta_copy().wait_send()
        for b in range(row_blocks):
            direct(b).wait_send()

    @pl.when(sec == last)
    def _():
        last_hop(0).wait_send()

    @pl.when(sec == half - 1)
    def _():
        last_hop(1).wait_send()

    @pl.when(sec == half)
    def _():
        last_hop(2).wait_send()

    @pl.when(sec == 0)
    def _():
        over().wait_send()
        across().wait_send()
        last_hop(3).wait_send()


def write(held, outbuf, wlast, normed, partial, kv_b, rebuilt, queries, keys_values, tail, sem):
    first = outbuf.shape[0]
    q_blocks = queries.shape[1] // COLS
    me = lax.axis_index("rep")
    x, y = me // 8, (me // 2) % 4
    side, quarter, late = quarters(x, y, normed.shape[1])

    def put(src, j):
        out, k = (queries, j) if j < q_blocks else (keys_values, j - q_blocks)
        return pltpu.make_async_copy(src, out.at[:, pl.ds(k * COLS, COLS)], sem.at[j])

    copies = [pltpu.make_async_copy(held, rebuilt, sem.at[first + GRP])]
    copies += [put(outbuf.at[j], j) for j in range(first)]
    for copy in copies:
        copy.start()
    cut = pl.ds(pl.multiple_of((1 - x) * side + late, BLK), quarter)
    for k in (0, 1, 2):
        if k == 0:
            total = jnp.dot(normed[...], wlast[k], preferred_element_type=jnp.float32)
        else:
            total = partial[k - 1] + jnp.dot(normed[:, cut], wlast[k, cut, :], preferred_element_type=jnp.float32)
        at = (first + k - q_blocks) * COLS
        tail[k] = (total + kv_b[:, at : at + COLS]).astype(jnp.bfloat16)
        copy = put(tail.at[k], first + k)
        copy.start()
        copies.append(copy)
    for copy in copies:
        copy.wait()


def body(
    cache, payload, block_ids, block_counts, block_scales, refresh_ids, refresh_counts,
    norm_gain, query_weight, query_bias, kv_weight, kv_bias,
):
    rows, feature = cache.shape[1:]
    depth, q_cols = query_weight.shape[1:]
    kv_cols = kv_weight.shape[2]
    blocks = (q_cols + kv_cols) // COLS
    groups = blocks // GRP
    row_blocks = rows // BLK

    anywhere = pl.BlockSpec(memory_space=pl.ANY)
    vmem = pl.BlockSpec(memory_space=pltpu.VMEM)
    dma = pltpu.SemaphoreType.DMA
    held, outbuf, wlast, normed, partial = pl.pallas_call(
        kernel,
        out_shape=(
            pltpu.VMEM((rows, feature), jnp.bfloat16),
            pltpu.VMEM((blocks - GRP, rows, COLS), jnp.bfloat16),
            pltpu.VMEM((GRP, feature, COLS), jnp.bfloat16),
            pltpu.VMEM((rows, feature), jnp.bfloat16),
            pltpu.VMEM((GRP - 1, rows, COLS), jnp.float32),
        ),
        in_specs=[anywhere, anywhere, vmem, vmem, vmem, vmem, vmem, vmem, anywhere, vmem, anywhere, vmem],
        out_specs=(vmem,) * 5,
        scratch_shapes=[
            pltpu.VMEM((blocks - GRP, feature, COLS), jnp.bfloat16),
            pltpu.VMEM((rows, feature), jnp.bfloat16),
            pltpu.VMEM((BLK, feature), jnp.bfloat16),
            pltpu.VMEM((BLK, feature), jnp.bfloat16),
            pltpu.VMEM((BLK, feature), jnp.bfloat16),
            pltpu.VMEM((8, BLK), jnp.int32),
            pltpu.VMEM((8, BLK), jnp.int32),
            pltpu.VMEM((1, q_cols + kv_cols), jnp.float32),
            dma((blocks,)),
            dma,
            dma((2,)),
            dma((CLASSES, groups)),
            dma((row_blocks,)),
            dma((row_blocks,)),
            dma,
            dma,
            dma,
            dma,
            dma,
            dma,
            dma,
            dma,
        ],
        compiler_params=pltpu.CompilerParams(collective_id=0, has_side_effects=True, vmem_limit_bytes=38 * 1024 * 1024),
        name="boundary",
    )(
        cache[0], payload[0], block_ids[0], block_counts, block_scales[0], refresh_ids[0], refresh_counts,
        norm_gain, query_weight[0], query_bias, kv_weight[0], kv_bias,
    )
    rebuilt, queries, keys_values = pl.pallas_call(
        write,
        out_shape=tuple(jax.ShapeDtypeStruct((rows, n), jnp.bfloat16) for n in (feature, q_cols, kv_cols)),
        in_specs=[vmem] * 6,
        out_specs=(anywhere, anywhere, anywhere),
        scratch_shapes=[pltpu.VMEM((GRP, rows, COLS), jnp.bfloat16), dma((blocks + 1,))],
        compiler_params=pltpu.CompilerParams(vmem_limit_bytes=4 * 1024 * 1024),
        name="write",
    )(held, outbuf, wlast, normed, partial, kv_bias)
    return rebuilt[None], queries[None], keys_values[None]


def solution(mesh):
    in_specs = (
        P("section", "rep", None),
        P("section", "rep", None),
        P("section", "rep", None),
        P("section", "rep"),
        P("section", "rep", None),
        P("section", "rep", None),
        P("section", "rep"),
        P("section", None),
        P("section", "rep", None),
        P("section", None),
        P("section", "rep", None),
        P("section", None),
    )
    out_specs = (P("section", "rep", None), P("section", "rep", None), P("section", "rep", None))
    return jax.shard_map(body, mesh=mesh, in_specs=in_specs, out_specs=out_specs, check_vma=False)
```

```python
import functools

import jax
import jax.numpy as jnp
from jax import lax
from jax.experimental import pallas as pl
from jax.experimental.pallas import tpu as pltpu
from jax.sharding import PartitionSpec as P

EPSILON = 1e-06
BLK = 128
COLS = 256
GRP = 3
MESH = pl.DeviceIdType.MESH

YM, YP, XP = 0, 1, 2
Y2B, Y2C, Y2A = 3, 4, 5
XYM_BC, XYP_BC, XYP_A, XYM_A = 6, 7, 8, 9
XY2B, XY2C, XY2A = 10, 11, 12
D_OWN, D_SIDE, D_FAR, D_A, D_Y2 = 13, 14, 15, 16, 17
CLASSES = 18


def quarters(x, y, extent):
    side = extent // 2
    return side, side // 2, (((y + 2) % 4) // 2) * (side // 2)


def kernel(
    cache, payload, ids_in, counts_in, scales_in, refresh_ids_in, refresh_counts_in, gain_in, q_w, q_b, kv_w, kv_b,
    held, outbuf, wlast, normed, partial,
    wbuf, pay, relay, relay_two, relay_three, meta, meta_in, bias,
    ld_sem, cache_sem, send, recv, pay_send, pay_recv, meta_send, meta_recv,
    ids, counts, scales, refresh_ids, refresh_counts, gain, small_sem,
    relay_send, relay_recv, two_send, two_recv, three_send, three_recv,
):
    sec = lax.axis_index("section")
    me = lax.axis_index("rep")
    depth = q_w.shape[0]
    q_blocks = q_w.shape[1] // COLS
    blocks = q_blocks + kv_w.shape[1] // COLS
    groups = blocks // GRP
    row_blocks = payload.shape[0] // BLK

    x, y, core = me // 8, (me // 2) % 4, me % 2

    def rank(dx, dy):
        return ((x + dx) % 2) * 8 + ((y + dy) % 4) * 2 + core

    ym, yp, y2 = rank(0, 3), rank(0, 1), rank(0, 2)
    xp, xym, xyp, xy2 = rank(1, 0), rank(1, 3), rank(1, 1), rank(1, 2)
    other = me + 1 - 2 * core

    split = blocks - GRP

    def part(first, count, start, size):
        buf, first = (wbuf, first) if first < split else (wlast, first - split)
        return buf.at[pl.ds(first, count), pl.ds(start, size), :]

    def region(r, first, count):
        return part(first, count, pl.multiple_of(r * depth, 32), depth)

    def remote(ref, cls, g, to):
        return pltpu.make_async_remote_copy(
            src_ref=ref, dst_ref=ref, send_sem=send.at[g // (groups - 1)], recv_sem=recv.at[cls, g],
            device_id=(sec, to), device_id_type=MESH,
        )

    sent = [0, 0]

    def push(r, first, count, cls, g, to):
        copy = remote(region(r, first, count), cls, g, to)
        copy.start()
        sent[g // (groups - 1)] += count

    def arrive(r, first, count, cls, g):
        remote(region(r, first, count), cls, g, other).wait_recv()

    last = lax.axis_size("section") - 1
    half = (last + 1) // 2
    barrier = pltpu.get_barrier_semaphore()

    def greet(to_sec, to_rep):
        pl.semaphore_signal(barrier, inc=1, device_id=(to_sec, to_rep), device_id_type=MESH)

    for r in (ym, yp, xp, other):
        greet(sec, r)
    expected = 4
    links = [(s + 1, s, me) for s in range(last)]
    links += [(0, half - 1, me), (last, half - 1, xp), (half, half - 1, xp), (half, last, xp), (half, 0, xp)]
    for receiver, sender, r in links:
        @pl.when(sec == receiver)
        def _():
            greet(sender, r)

        expected = expected + jnp.where(sec == sender, 1, 0)

    loads = []
    for j in range(blocks):
        if j < q_blocks:
            src = q_w.at[:, pl.ds(j * COLS, COLS)]
        else:
            src = kv_w.at[:, pl.ds((j - q_blocks) * COLS, COLS)]
        buf, k = (wbuf, j) if j < split else (wlast, j - split)
        rows = pl.ds(pl.multiple_of(me * depth, 32), depth)
        copy = pltpu.make_async_copy(src, buf.at[k, rows, :], ld_sem.at[j])
        copy.start()
        loads.append(copy)

    q_cols = q_w.shape[1]
    small = [
        pltpu.make_async_copy(src, dst, small_sem.at[i])
        for i, (src, dst) in enumerate(
            (
                (ids_in, ids), (counts_in, counts), (scales_in, scales), (refresh_ids_in, refresh_ids),
                (refresh_counts_in, refresh_counts), (gain_in, gain),
                (q_b, bias.at[:, pl.ds(0, q_cols)]), (kv_b, bias.at[:, pl.ds(q_cols, kv_w.shape[1])]),
            )
        )
    ]
    for copy in small:
        copy.start()
    load_cache = pltpu.make_async_copy(cache, held, cache_sem)
    load_cache.start()

    for copy in small:
        copy.wait()

    lane = lax.broadcasted_iota(jnp.int32, (1, BLK), 1)

    def two(v):
        return jnp.where(lane == 0, v[:, 0:1], v[:, 1:2])

    meta[0:1, :] = refresh_ids[...]
    meta[1:2, :] = jnp.broadcast_to(refresh_counts[...], (1, BLK))
    meta[2:3, :] = two(ids[...])
    meta[3:4, :] = two(scales[...])
    meta[4:5, :] = jnp.broadcast_to(counts[...], (1, BLK))
    meta[5:8, :] = jnp.zeros((3, BLK), jnp.int32)

    pl.semaphore_wait(barrier, expected)

    def block(ref, b):
        return ref.at[pl.ds(b * BLK, BLK), :]

    def pay_copy(src, dst, to_sec, to_rep, send_sem, recv_sem):
        return pltpu.make_async_remote_copy(
            src_ref=src, dst_ref=dst, send_sem=send_sem, recv_sem=recv_sem,
            device_id=(to_sec, to_rep), device_id_type=MESH,
        )

    following = lax.rem(sec + 1, last + 1)

    def direct(b):
        return pay_copy(block(payload, b), block(pay, b), following, me, pay_send.at[b], pay_recv.at[b])

    def first_hop(b):
        to_sec, to_rep = ((last, xp), (half - 1, xp), (0, me), (0, me))[b]
        dst, sem = (relay_two, two_recv) if b == 3 else (relay, relay_recv)
        return pay_copy(block(payload, b), dst, to_sec, to_rep, pay_send.at[b], sem)

    def over():
        return pay_copy(relay, relay, half, xp, relay_send, relay_recv)

    def across():
        return pay_copy(relay_two, relay_three, 0, xp, two_send, three_recv)

    def last_hop(b):
        src, sem = (relay_three, three_send) if b == 3 else (relay, relay_send)
        return pay_copy(src, block(pay, b), half, xp, sem, pay_recv.at[b])

    def relay_first():
        @pl.when(sec == last)
        def _():
            first_hop(0).wait_recv()
            last_hop(0).start()

        @pl.when(sec == 0)
        def _():
            first_hop(2).wait_recv()
            over().start()

    def relay_second():
        @pl.when(sec == half - 1)
        def _():
            first_hop(1).wait_recv()
            last_hop(1).start()

        @pl.when(sec == half)
        def _():
            over().wait_recv()
            last_hop(2).start()

        @pl.when(sec == 0)
        def _():
            first_hop(3).wait_recv()
            across().start()

    def relay_third():
        @pl.when(sec == 0)
        def _():
            across().wait_recv()
            last_hop(3).start()

    def meta_copy():
        return pay_copy(meta, meta_in, following, me, meta_send, meta_recv)

    @pl.when(sec != last)
    def _():
        meta_copy().start()

    @pl.when(sec == half - 1)
    def _():
        for b in (0, 2, 3):
            first_hop(b).start()

    @pl.when((sec != half - 1) & (sec != last))
    def _():
        for b in range(row_blocks):
            direct(b).start()

    def fill(b):
        return pltpu.make_async_copy(block(payload, b), block(pay, b), pay_recv.at[b])

    @pl.when(sec == 0)
    def _():
        meta_in[...] = jnp.zeros((8, BLK), jnp.int32)
        for b in range(row_blocks):
            fill(b).start()

    def own_x(g):
        push(me, g * GRP, GRP, XP, g, xp)

    for g in range(groups):
        for j in range(g * GRP, (g + 1) * GRP):
            loads[j].wait()
        push(me, g * GRP, GRP, YM, g, yp)
        push(me, g * GRP, GRP, YP, g, ym)
        if g < groups // 2:
            own_x(g)
        if g == 1:
            @pl.when(sec == half - 1)
            def _():
                first_hop(1).start()

        push(me, g * GRP, GRP, D_OWN, g, other)

    def level1(g):
        a = g * GRP
        there, source = (yp, ym) if g % 2 == 0 else (ym, yp)
        final = g == groups - 1
        arrive(ym, a, GRP, YM, g)
        arrive(yp, a, GRP, YP, g)
        if final:
            push(source, a, 1, Y2A, g, there)
        arrive(xp, a, GRP, XP, g)
        push(xp, a + 1, 2, XYM_BC, g, yp)
        push(xp, a + 1, 2, XYP_BC, g, ym)
        push(ym, a + 1, 1, Y2B, g, yp)
        push(yp, a + 2, 1, Y2C, g, ym)
        if not final:
            push(source, a, 1, Y2A, g, there)
        push(xp, a, GRP, D_OWN, g, other)
        push(ym, a, GRP, D_OWN, g, other)
        push(yp, a, GRP, D_OWN, g, other)

    def beside(g):
        push(ym, g * GRP, 1, XYM_A, g, xp)
        push(yp, g * GRP, 1, XYP_A, g, xp)

    def level2_up(g):
        arrive(xym, g * GRP + 1, 2, XYM_BC, g)
        push(xym, g * GRP + 1, 1, XY2B, g, yp)
        push(xym, g * GRP + 1, 2, D_SIDE, g, other)

    def level2_down(g):
        arrive(xyp, g * GRP + 1, 2, XYP_BC, g)
        push(xyp, g * GRP + 2, 1, XY2C, g, ym)
        push(xyp, g * GRP + 1, 2, D_SIDE, g, other)

    def level2(g):
        level2_up(g)
        level2_down(g)

    def opposite_a(g):
        arrive(y2, g * GRP, 1, Y2A, g)
        push(y2, g * GRP, 1, XY2A, g, xp)

    def opposite(g):
        a = g * GRP
        arrive(y2, a + 1, 1, Y2B, g)
        arrive(y2, a + 2, 1, Y2C, g)
        push(y2, a, GRP, D_Y2, g, other)

    def far(g):
        a = g * GRP
        arrive(xy2, a + 1, 1, XY2B, g)
        arrive(xy2, a + 2, 1, XY2C, g)
        push(xy2, a + 1, 2, D_FAR, g, other)

    def sides(g):
        a = g * GRP
        arrive(xym, a, 1, XYM_A, g)
        push(xym, a, 1, D_A, g, other)
        arrive(xyp, a, 1, XYP_A, g)
        push(xyp, a, 1, D_A, g, other)
        arrive(xy2, a, 1, XY2A, g)
        push(xy2, a, 1, D_A, g, other)

    valid = sec > 0

    def rebuild(b):
        @pl.when(sec != 0)
        def _():
            direct(b).wait_recv()

        @pl.when(sec == 0)
        def _():
            fill(b).wait()

        lists = meta_in[...]
        refreshed = jnp.where((lane < lists[1:2, :]) & valid, lists[0:1, :], -1)
        listed = (lane < lists[4:5, :]) & (lane < ids.shape[1]) & (lists[2:3, :] == b) & valid
        factor = jnp.sum(jnp.where(listed, lists[3:4, :].astype(jnp.float32) / 4096.0, 0.0), axis=1, keepdims=True)
        strip = 16

        def one(i, carry):
            start = pl.multiple_of(b * BLK + i * strip, strip)
            rows = pl.ds(start, strip)
            number = lax.broadcasted_iota(jnp.int32, (strip, BLK), 0) + start
            hit = jnp.max(jnp.where(number == refreshed, 1.0, 0.0), axis=1, keepdims=True) > 0.0
            came = pay[rows, :].astype(jnp.float32)
            delta = (came * factor).astype(jnp.bfloat16).astype(jnp.float32)
            mixed = jnp.where(hit, came, held[rows, :].astype(jnp.float32) + delta).astype(jnp.bfloat16)
            held[rows, :] = mixed
            wide = mixed.astype(jnp.float32)
            scale = lax.rsqrt(jnp.mean(wide * wide, axis=1, keepdims=True) + EPSILON)
            normed[rows, :] = (wide * scale * gain[...]).astype(jnp.bfloat16)
            return carry

        lax.fori_loop(0, BLK // strip, one, 0)

    once = jnp.where(me >= 0, 1, 0)

    def product(buf, j, start, size):
        cut = pl.ds(pl.multiple_of(start, BLK), size)
        return jnp.dot(normed[:, cut], buf[j, cut, :], preferred_element_type=jnp.float32)

    def finish(j, total):
        cols = pl.ds(pl.multiple_of(j * COLS, COLS), COLS)
        outbuf[j] = (total + bias[:, cols]).astype(jnp.bfloat16)

    def handed(first, count, shards, cls, g):
        remote(part(first, count, 0, shards * depth), cls, g, other).wait_recv()

    def near(g):
        handed(g * GRP, GRP, 4, D_OWN, g)
        handed(g * GRP + 1, 2, 2, D_SIDE, g)

    def pair_ready(g):
        near(g)
        handed(g * GRP, GRP, 1, D_Y2, g)
        handed(g * GRP + 1, 2, 1, D_FAR, g)

    def multiply(first, count):
        def one(j, carry):
            finish(j, product(wbuf, j, 0, normed.shape[1]))
            return carry

        lax.fori_loop(first, first + count * once, one, 0)

    def pair(g):
        pair_ready(g)
        multiply(g * GRP + 1, 2)

    def single(g):
        handed(g * GRP, 1, 3, D_A, g)
        multiply(g * GRP, 1)

    side, quarter, late = quarters(x, y, normed.shape[1])
    mine, yours, soon = x * side, (1 - x) * side, quarter - late

    def prepare(g):
        near(g)

        def one(k, carry):
            partial[k] = product(wlast, 1 + k, mine + soon, quarter) + product(wlast, 1 + k, yours + soon, quarter)
            return carry

        lax.fori_loop(0, GRP - 1, one, 0)

    def extend(g):
        handed(g * GRP, GRP, 1, D_Y2, g)

        def one(k, carry):
            partial[k] += product(wlast, 1 + k, mine + late, quarter)
            return carry

        lax.fori_loop(0, GRP - 1, one, 0)

    level1(0)
    level1(1)
    relay_first()
    own_x(3)
    beside(0)
    beside(1)
    relay_second()
    own_x(4)
    load_cache.wait()

    @pl.when(sec != 0)
    def _():
        meta_copy().wait_recv()

    level2(0)
    level1(2)
    beside(2)
    opposite_a(0)
    opposite(0)
    own_x(5)
    rebuild(0)
    relay_third()
    level2(1)
    level1(3)
    beside(3)
    opposite_a(1)
    opposite(1)
    far(0)
    rebuild(1)
    level2(2)
    level1(4)
    beside(4)
    opposite_a(2)
    opposite(2)
    far(1)
    rebuild(2)
    rebuild(3)
    pair(0)
    level2(3)
    opposite_a(3)
    opposite(3)
    sides(0)
    pair(1)
    far(2)
    single(0)
    pair(2)
    sides(1)
    level2(4)
    level1(5)
    beside(5)
    single(1)
    opposite_a(4)
    opposite(4)
    far(3)
    far(4)
    sides(2)
    pair(3)
    opposite_a(5)
    sides(3)
    single(2)
    pair_ready(4)
    multiply(4 * GRP + 1, 1)
    level2_up(5)
    multiply(4 * GRP + 2, 1)
    level2_down(5)
    single(3)
    opposite(5)
    prepare(5)
    far(5)
    sides(4)
    extend(5)
    sides(5)
    single(4)
    handed(5 * GRP + 1, 2, 1, D_FAR, 5)
    handed(5 * GRP, 1, 3, D_A, 5)

    for k, buf in enumerate((wbuf, wlast)):
        slabs, left = divmod(sent[k], buf.shape[0])
        assert left == 0
        everything = buf.at[:, pl.ds(0, slabs * depth), :]
        pltpu.make_async_remote_copy(
            src_ref=everything, dst_ref=everything, send_sem=send.at[k], recv_sem=recv.at[0, 0],
            device_id=(sec, other), device_id_type=MESH,
        ).wait_send()

    @pl.when(sec != last)
    def _():
        meta_copy().wait_send()
        for b in range(row_blocks):
            direct(b).wait_send()

    @pl.when(sec == last)
    def _():
        last_hop(0).wait_send()

    @pl.when(sec == half - 1)
    def _():
        last_hop(1).wait_send()

    @pl.when(sec == half)
    def _():
        last_hop(2).wait_send()

    @pl.when(sec == 0)
    def _():
        over().wait_send()
        across().wait_send()
        last_hop(3).wait_send()


def write(held, outbuf, wlast, normed, partial, kv_b, rebuilt, queries, keys_values, tail, sem):
    first = outbuf.shape[0]
    q_blocks = queries.shape[1] // COLS
    me = lax.axis_index("rep")
    x, y = me // 8, (me // 2) % 4
    side, quarter, late = quarters(x, y, normed.shape[1])

    def put(src, j):
        out, k = (queries, j) if j < q_blocks else (keys_values, j - q_blocks)
        return pltpu.make_async_copy(src, out.at[:, pl.ds(k * COLS, COLS)], sem.at[j])

    copies = [pltpu.make_async_copy(held, rebuilt, sem.at[first + GRP])]
    copies += [put(outbuf.at[j], j) for j in range(first)]
    for copy in copies:
        copy.start()
    cut = pl.ds(pl.multiple_of((1 - x) * side + late, BLK), quarter)
    for k in (0, 1, 2):
        if k == 0:
            total = jnp.dot(normed[...], wlast[k], preferred_element_type=jnp.float32)
        else:
            total = partial[k - 1] + jnp.dot(normed[:, cut], wlast[k, cut, :], preferred_element_type=jnp.float32)
        at = (first + k - q_blocks) * COLS
        tail[k] = (total + kv_b[:, at : at + COLS]).astype(jnp.bfloat16)
        copy = put(tail.at[k], first + k)
        copy.start()
        copies.append(copy)
    for copy in copies:
        copy.wait()


def body(
    cache, payload, block_ids, block_counts, block_scales, refresh_ids, refresh_counts,
    norm_gain, query_weight, query_bias, kv_weight, kv_bias,
):
    rows, feature = cache.shape[1:]
    depth, q_cols = query_weight.shape[1:]
    kv_cols = kv_weight.shape[2]
    blocks = (q_cols + kv_cols) // COLS
    groups = blocks // GRP
    row_blocks = rows // BLK

    anywhere = pl.BlockSpec(memory_space=pl.ANY)
    vmem = pl.BlockSpec(memory_space=pltpu.VMEM)
    dma = pltpu.SemaphoreType.DMA
    held, outbuf, wlast, normed, partial = pl.pallas_call(
        kernel,
        out_shape=(
            pltpu.VMEM((rows, feature), jnp.bfloat16),
            pltpu.VMEM((blocks - GRP, rows, COLS), jnp.bfloat16),
            pltpu.VMEM((GRP, feature, COLS), jnp.bfloat16),
            pltpu.VMEM((rows, feature), jnp.bfloat16),
            pltpu.VMEM((GRP - 1, rows, COLS), jnp.float32),
        ),
        in_specs=[anywhere] * 12,
        out_specs=(vmem,) * 5,
        scratch_shapes=[
            pltpu.VMEM((blocks - GRP, feature, COLS), jnp.bfloat16),
            pltpu.VMEM((rows, feature), jnp.bfloat16),
            pltpu.VMEM((BLK, feature), jnp.bfloat16),
            pltpu.VMEM((BLK, feature), jnp.bfloat16),
            pltpu.VMEM((BLK, feature), jnp.bfloat16),
            pltpu.VMEM((8, BLK), jnp.int32),
            pltpu.VMEM((8, BLK), jnp.int32),
            pltpu.VMEM((1, q_cols + kv_cols), jnp.float32),
            dma((blocks,)),
            dma,
            dma((2,)),
            dma((CLASSES, groups)),
            dma((row_blocks,)),
            dma((row_blocks,)),
            dma,
            dma,
            pltpu.VMEM(block_ids.shape[1:], jnp.int32),
            pltpu.VMEM(block_counts.shape, jnp.int32),
            pltpu.VMEM(block_scales.shape[1:], jnp.int32),
            pltpu.VMEM(refresh_ids.shape[1:], jnp.int32),
            pltpu.VMEM(refresh_counts.shape, jnp.int32),
            pltpu.VMEM(norm_gain.shape, jnp.float32),
            dma((8,)),
            dma,
            dma,
            dma,
            dma,
            dma,
            dma,
        ],
        compiler_params=pltpu.CompilerParams(collective_id=0, has_side_effects=True, vmem_limit_bytes=38 * 1024 * 1024),
        name="boundary",
    )(
        cache[0], payload[0], block_ids[0], block_counts, block_scales[0], refresh_ids[0], refresh_counts,
        norm_gain, query_weight[0], query_bias, kv_weight[0], kv_bias,
    )
    rebuilt, queries, keys_values = pl.pallas_call(
        write,
        out_shape=tuple(jax.ShapeDtypeStruct((rows, n), jnp.bfloat16) for n in (feature, q_cols, kv_cols)),
        in_specs=[vmem] * 6,
        out_specs=(anywhere, anywhere, anywhere),
        scratch_shapes=[pltpu.VMEM((GRP, rows, COLS), jnp.bfloat16), dma((blocks + 1,))],
        compiler_params=pltpu.CompilerParams(vmem_limit_bytes=4 * 1024 * 1024),
        name="write",
    )(held, outbuf, wlast, normed, partial, kv_bias)
    return rebuilt[None], queries[None], keys_values[None]


def solution(mesh):
    in_specs = (
        P("section", "rep", None),
        P("section", "rep", None),
        P("section", "rep", None),
        P("section", "rep"),
        P("section", "rep", None),
        P("section", "rep", None),
        P("section", "rep"),
        P("section", None),
        P("section", "rep", None),
        P("section", None),
        P("section", "rep", None),
        P("section", None),
    )
    out_specs = (P("section", "rep", None), P("section", "rep", None), P("section", "rep", None))
    return jax.shard_map(body, mesh=mesh, in_specs=in_specs, out_specs=out_specs, check_vma=False)
```

```python
import functools

import jax
import jax.numpy as jnp
from jax import lax
from jax.experimental import pallas as pl
from jax.experimental.pallas import tpu as pltpu
from jax.sharding import PartitionSpec as P

EPSILON = 1e-06
BLK = 128
COLS = 256
GRP = 3
MESH = pl.DeviceIdType.MESH

YM, YP, XP = 0, 1, 2
Y2B, Y2C, Y2A = 3, 4, 5
XYM_BC, XYP_BC, XYP_A, XYM_A = 6, 7, 8, 9
XY2B, XY2C, XY2A = 10, 11, 12
D_OWN, D_SIDE, D_FAR, D_A, D_Y2 = 13, 14, 15, 16, 17
CLASSES = 18


def quarters(x, y, extent):
    side = extent // 2
    return side, side // 2, (((y + 2) % 4) // 2) * (side // 2)


def kernel(
    cache, payload, ids_in, counts_in, scales_in, refresh_ids_in, refresh_counts_in, gain_in, q_w, q_b, kv_w, kv_b,
    held, outbuf, wlast, normed, partial,
    wbuf, pay, relay, relay_two, relay_three, meta, meta_in, bias,
    ld_sem, cache_sem, send, recv, pay_send, pay_recv, meta_send, meta_recv,
    ids, counts, scales, refresh_ids, refresh_counts, gain, small_sem,
    relay_send, relay_recv, two_send, two_recv, three_send, three_recv,
):
    sec = lax.axis_index("section")
    me = lax.axis_index("rep")
    depth = q_w.shape[0]
    q_blocks = q_w.shape[1] // COLS
    blocks = q_blocks + kv_w.shape[1] // COLS
    groups = blocks // GRP
    row_blocks = payload.shape[0] // BLK

    x, y, core = me // 8, (me // 2) % 4, me % 2

    def rank(dx, dy):
        return ((x + dx) % 2) * 8 + ((y + dy) % 4) * 2 + core

    ym, yp, y2 = rank(0, 3), rank(0, 1), rank(0, 2)
    xp, xym, xyp, xy2 = rank(1, 0), rank(1, 3), rank(1, 1), rank(1, 2)
    other = me + 1 - 2 * core

    split = blocks - GRP

    def part(first, count, start, size):
        buf, first = (wbuf, first) if first < split else (wlast, first - split)
        return buf.at[pl.ds(first, count), pl.ds(start, size), :]

    def region(r, first, count):
        return part(first, count, pl.multiple_of(r * depth, 32), depth)

    def remote(ref, cls, g, to):
        return pltpu.make_async_remote_copy(
            src_ref=ref, dst_ref=ref, send_sem=send.at[g // (groups - 1)], recv_sem=recv.at[cls, g],
            device_id=(sec, to), device_id_type=MESH,
        )

    sent = [0, 0]

    def push(r, first, count, cls, g, to):
        copy = remote(region(r, first, count), cls, g, to)
        copy.start()
        sent[g // (groups - 1)] += count

    def arrive(r, first, count, cls, g):
        remote(region(r, first, count), cls, g, other).wait_recv()

    last = lax.axis_size("section") - 1
    half = (last + 1) // 2
    barrier = pltpu.get_barrier_semaphore()

    def greet(to_sec, to_rep):
        pl.semaphore_signal(barrier, inc=1, device_id=(to_sec, to_rep), device_id_type=MESH)

    for r in (ym, yp, xp, other):
        greet(sec, r)
    expected = 4
    links = [(s + 1, s, me) for s in range(last)]
    links += [(0, half - 1, me), (last, half - 1, xp), (half, half - 1, xp), (half, last, xp), (half, 0, xp)]
    for receiver, sender, r in links:
        @pl.when(sec == receiver)
        def _():
            greet(sender, r)

        expected = expected + jnp.where(sec == sender, 1, 0)

    loads = []
    for j in range(blocks):
        if j < q_blocks:
            src = q_w.at[:, pl.ds(j * COLS, COLS)]
        else:
            src = kv_w.at[:, pl.ds((j - q_blocks) * COLS, COLS)]
        buf, k = (wbuf, j) if j < split else (wlast, j - split)
        rows = pl.ds(pl.multiple_of(me * depth, 32), depth)
        copy = pltpu.make_async_copy(src, buf.at[k, rows, :], ld_sem.at[j])
        copy.start()
        loads.append(copy)

    q_cols = q_w.shape[1]
    small = [
        pltpu.make_async_copy(src, dst, small_sem.at[i])
        for i, (src, dst) in enumerate(
            (
                (ids_in, ids), (counts_in, counts), (scales_in, scales), (refresh_ids_in, refresh_ids),
                (refresh_counts_in, refresh_counts), (gain_in, gain),
                (q_b, bias.at[:, pl.ds(0, q_cols)]), (kv_b, bias.at[:, pl.ds(q_cols, kv_w.shape[1])]),
            )
        )
    ]
    for copy in small:
        copy.start()
    load_cache = pltpu.make_async_copy(cache, held, cache_sem)
    load_cache.start()

    for copy in small:
        copy.wait()

    lane = lax.broadcasted_iota(jnp.int32, (1, BLK), 1)

    def two(v):
        return jnp.where(lane == 0, v[:, 0:1], v[:, 1:2])

    meta[0:1, :] = refresh_ids[...]
    meta[1:2, :] = jnp.broadcast_to(refresh_counts[...], (1, BLK))
    meta[2:3, :] = two(ids[...])
    meta[3:4, :] = two(scales[...])
    meta[4:5, :] = jnp.broadcast_to(counts[...], (1, BLK))
    meta[5:8, :] = jnp.zeros((3, BLK), jnp.int32)

    pl.semaphore_wait(barrier, expected)

    def block(ref, b):
        return ref.at[pl.ds(b * BLK, BLK), :]

    def pay_copy(src, dst, to_sec, to_rep, send_sem, recv_sem):
        return pltpu.make_async_remote_copy(
            src_ref=src, dst_ref=dst, send_sem=send_sem, recv_sem=recv_sem,
            device_id=(to_sec, to_rep), device_id_type=MESH,
        )

    following = lax.rem(sec + 1, last + 1)

    def direct(b):
        return pay_copy(block(payload, b), block(pay, b), following, me, pay_send.at[b], pay_recv.at[b])

    def first_hop(b):
        to_sec, to_rep = ((last, xp), (half - 1, xp), (0, me), (0, me))[b]
        dst, sem = (relay_two, two_recv) if b == 3 else (relay, relay_recv)
        return pay_copy(block(payload, b), dst, to_sec, to_rep, pay_send.at[b], sem)

    def over():
        return pay_copy(relay, relay, half, xp, relay_send, relay_recv)

    def across():
        return pay_copy(relay_two, relay_three, 0, xp, two_send, three_recv)

    def last_hop(b):
        src, sem = (relay_three, three_send) if b == 3 else (relay, relay_send)
        return pay_copy(src, block(pay, b), half, xp, sem, pay_recv.at[b])

    def relay_first():
        @pl.when(sec == last)
        def _():
            first_hop(0).wait_recv()
            last_hop(0).start()

        @pl.when(sec == 0)
        def _():
            first_hop(2).wait_recv()
            over().start()

    def relay_second():
        @pl.when(sec == half - 1)
        def _():
            first_hop(1).wait_recv()
            last_hop(1).start()

        @pl.when(sec == half)
        def _():
            over().wait_recv()
            last_hop(2).start()

        @pl.when(sec == 0)
        def _():
            first_hop(3).wait_recv()
            across().start()

    def relay_third():
        @pl.when(sec == 0)
        def _():
            across().wait_recv()
            last_hop(3).start()

    def meta_copy():
        return pay_copy(meta, meta_in, following, me, meta_send, meta_recv)

    @pl.when(sec != last)
    def _():
        meta_copy().start()

    @pl.when(sec == half - 1)
    def _():
        for b in (0, 2, 3):
            first_hop(b).start()

    @pl.when((sec != half - 1) & (sec != last))
    def _():
        for b in range(row_blocks):
            direct(b).start()

    def fill(b):
        return pltpu.make_async_copy(block(payload, b), block(pay, b), pay_recv.at[b])

    @pl.when(sec == 0)
    def _():
        meta_in[...] = jnp.zeros((8, BLK), jnp.int32)
        for b in range(row_blocks):
            fill(b).start()

    def own_x(g):
        push(me, g * GRP, GRP, XP, g, xp)

    for g in range(groups):
        for j in range(g * GRP, (g + 1) * GRP):
            loads[j].wait()
        push(me, g * GRP, GRP, YM, g, yp)
        push(me, g * GRP, GRP, YP, g, ym)
        if g < groups // 2:
            own_x(g)
        if g == 1:
            @pl.when(sec == half - 1)
            def _():
                first_hop(1).start()

        push(me, g * GRP, GRP, D_OWN, g, other)

    def level1(g):
        a = g * GRP
        there, source = (yp, ym) if g % 2 == 0 else (ym, yp)
        final = g == groups - 1
        arrive(ym, a, GRP, YM, g)
        arrive(yp, a, GRP, YP, g)
        if final:
            push(source, a, 1, Y2A, g, there)
        arrive(xp, a, GRP, XP, g)
        push(xp, a + 1, 2, XYM_BC, g, yp)
        push(xp, a + 1, 2, XYP_BC, g, ym)
        push(ym, a + 1, 1, Y2B, g, yp)
        push(yp, a + 2, 1, Y2C, g, ym)
        if not final:
            push(source, a, 1, Y2A, g, there)
        push(xp, a, GRP, D_OWN, g, other)
        push(ym, a, GRP, D_OWN, g, other)
        push(yp, a, GRP, D_OWN, g, other)

    def beside(g):
        push(ym, g * GRP, 1, XYM_A, g, xp)
        push(yp, g * GRP, 1, XYP_A, g, xp)

    def level2_up(g):
        arrive(xym, g * GRP + 1, 2, XYM_BC, g)
        push(xym, g * GRP + 1, 1, XY2B, g, yp)
        push(xym, g * GRP + 1, 2, D_SIDE, g, other)

    def level2_down(g):
        arrive(xyp, g * GRP + 1, 2, XYP_BC, g)
        push(xyp, g * GRP + 2, 1, XY2C, g, ym)
        push(xyp, g * GRP + 1, 2, D_SIDE, g, other)

    def level2(g):
        level2_up(g)
        level2_down(g)

    def opposite_a(g):
        arrive(y2, g * GRP, 1, Y2A, g)
        push(y2, g * GRP, 1, XY2A, g, xp)

    def opposite(g):
        a = g * GRP
        arrive(y2, a + 1, 1, Y2B, g)
        arrive(y2, a + 2, 1, Y2C, g)
        push(y2, a, GRP, D_Y2, g, other)

    def far(g):
        a = g * GRP
        arrive(xy2, a + 1, 1, XY2B, g)
        arrive(xy2, a + 2, 1, XY2C, g)
        push(xy2, a + 1, 2, D_FAR, g, other)

    def sides(g):
        a = g * GRP
        arrive(xym, a, 1, XYM_A, g)
        push(xym, a, 1, D_A, g, other)
        arrive(xyp, a, 1, XYP_A, g)
        push(xyp, a, 1, D_A, g, other)
        arrive(xy2, a, 1, XY2A, g)
        push(xy2, a, 1, D_A, g, other)

    valid = sec > 0

    def rebuild(b):
        @pl.when(sec != 0)
        def _():
            direct(b).wait_recv()

        @pl.when(sec == 0)
        def _():
            fill(b).wait()

        lists = meta_in[...]
        refreshed = jnp.where((lane < lists[1:2, :]) & valid, lists[0:1, :], -1)
        listed = (lane < lists[4:5, :]) & (lane < ids.shape[1]) & (lists[2:3, :] == b) & valid
        factor = jnp.sum(jnp.where(listed, lists[3:4, :].astype(jnp.float32) / 4096.0, 0.0), axis=1, keepdims=True)
        strip = 16

        def one(i, carry):
            start = pl.multiple_of(b * BLK + i * strip, strip)
            rows = pl.ds(start, strip)
            number = lax.broadcasted_iota(jnp.int32, (strip, BLK), 0) + start
            hit = jnp.max(jnp.where(number == refreshed, 1.0, 0.0), axis=1, keepdims=True) > 0.0
            came = pay[rows, :].astype(jnp.float32)
            delta = (came * factor).astype(jnp.bfloat16).astype(jnp.float32)
            mixed = jnp.where(hit, came, held[rows, :].astype(jnp.float32) + delta).astype(jnp.bfloat16)
            held[rows, :] = mixed
            wide = mixed.astype(jnp.float32)
            scale = lax.rsqrt(jnp.mean(wide * wide, axis=1, keepdims=True) + EPSILON)
            normed[rows, :] = (wide * scale * gain[...]).astype(jnp.bfloat16)
            return carry

        lax.fori_loop(0, BLK // strip, one, 0)

    once = jnp.where(me >= 0, 1, 0)

    def product(buf, j, start, size):
        cut = pl.ds(pl.multiple_of(start, BLK), size)
        return jnp.dot(normed[:, cut], buf[j, cut, :], preferred_element_type=jnp.float32)

    def finish(j, total):
        cols = pl.ds(pl.multiple_of(j * COLS, COLS), COLS)
        outbuf[j] = (total + bias[:, cols]).astype(jnp.bfloat16)

    def handed(first, count, shards, cls, g):
        remote(part(first, count, 0, shards * depth), cls, g, other).wait_recv()

    def near(g):
        handed(g * GRP, GRP, 4, D_OWN, g)
        handed(g * GRP + 1, 2, 2, D_SIDE, g)

    def pair_ready(g):
        near(g)
        handed(g * GRP, GRP, 1, D_Y2, g)
        handed(g * GRP + 1, 2, 1, D_FAR, g)

    def multiply(first, count):
        def one(j, carry):
            finish(j, product(wbuf, j, 0, normed.shape[1]))
            return carry

        lax.fori_loop(first, first + count * once, one, 0)

    def pair(g):
        pair_ready(g)
        multiply(g * GRP + 1, 2)

    def single(g):
        handed(g * GRP, 1, 3, D_A, g)
        multiply(g * GRP, 1)

    side, quarter, late = quarters(x, y, normed.shape[1])
    mine, yours, soon = x * side, (1 - x) * side, quarter - late

    def prepare(g):
        near(g)

        def one(k, carry):
            partial[k] = product(wlast, 1 + k, mine + soon, quarter) + product(wlast, 1 + k, yours + soon, quarter)
            return carry

        lax.fori_loop(0, GRP - 1, one, 0)

    def extend(g):
        handed(g * GRP, GRP, 1, D_Y2, g)

        def one(k, carry):
            partial[k] += product(wlast, 1 + k, mine + late, quarter)
            return carry

        lax.fori_loop(0, GRP - 1, one, 0)

    level1(0)
    level1(1)
    relay_first()
    own_x(3)
    beside(0)
    beside(1)
    relay_second()
    own_x(4)
    load_cache.wait()

    @pl.when(sec != 0)
    def _():
        meta_copy().wait_recv()

    level2(0)
    level1(2)
    beside(2)
    opposite_a(0)
    opposite(0)
    own_x(5)
    rebuild(0)
    relay_third()
    level2(1)
    level1(3)
    beside(3)
    opposite_a(1)
    opposite(1)
    far(0)
    rebuild(1)
    level2(2)
    level1(4)
    beside(4)
    opposite_a(2)
    opposite(2)
    far(1)
    rebuild(2)
    rebuild(3)
    pair(0)
    level2(3)
    opposite_a(3)
    opposite(3)
    sides(0)
    pair(1)
    far(2)
    single(0)
    pair(2)
    sides(1)
    level2(4)
    level1(5)
    beside(5)
    single(1)
    opposite_a(4)
    opposite(4)
    far(3)
    far(4)
    sides(2)
    pair(3)
    opposite_a(5)
    sides(3)
    single(2)
    pair_ready(4)
    multiply(4 * GRP + 1, 1)
    level2_up(5)
    multiply(4 * GRP + 2, 1)
    level2_down(5)
    single(3)
    opposite(5)
    prepare(5)
    far(5)
    sides(4)
    extend(5)
    sides(5)
    single(4)
    handed(5 * GRP + 1, 2, 1, D_FAR, 5)
    handed(5 * GRP, 1, 3, D_A, 5)

    for k, buf in enumerate((wbuf, wlast)):
        slabs, left = divmod(sent[k], buf.shape[0])
        assert left == 0
        everything = buf.at[:, pl.ds(0, slabs * depth), :]
        pltpu.make_async_remote_copy(
            src_ref=everything, dst_ref=everything, send_sem=send.at[k], recv_sem=recv.at[0, 0],
            device_id=(sec, other), device_id_type=MESH,
        ).wait_send()

    @pl.when(sec != last)
    def _():
        meta_copy().wait_send()
        for b in range(row_blocks):
            direct(b).wait_send()

    @pl.when(sec == last)
    def _():
        last_hop(0).wait_send()

    @pl.when(sec == half - 1)
    def _():
        last_hop(1).wait_send()

    @pl.when(sec == half)
    def _():
        last_hop(2).wait_send()

    @pl.when(sec == 0)
    def _():
        over().wait_send()
        across().wait_send()
        last_hop(3).wait_send()


def write(held, outbuf, wlast, normed, partial, kv_b, rebuilt, queries, keys_values, tail, sem):
    first = outbuf.shape[0]
    q_blocks = queries.shape[1] // COLS
    me = lax.axis_index("rep")
    x, y = me // 8, (me // 2) % 4
    side, quarter, late = quarters(x, y, normed.shape[1])

    def put(src, j):
        out, k = (queries, j) if j < q_blocks else (keys_values, j - q_blocks)
        return pltpu.make_async_copy(src, out.at[:, pl.ds(k * COLS, COLS)], sem.at[j])

    copies = []
    for b in range(held.shape[0] // BLK):
        rows = pl.ds(b * BLK, BLK)
        copies.append(pltpu.make_async_copy(held.at[rows, :], rebuilt.at[rows, :], sem.at[first + GRP + b]))
    copies += [put(outbuf.at[j], j) for j in range(first)]
    for copy in copies:
        copy.start()
    cut = pl.ds(pl.multiple_of((1 - x) * side + late, BLK), quarter)
    for k in (0, 1, 2):
        if k == 0:
            total = jnp.dot(normed[...], wlast[k], preferred_element_type=jnp.float32)
        else:
            total = partial[k - 1] + jnp.dot(normed[:, cut], wlast[k, cut, :], preferred_element_type=jnp.float32)
        at = (first + k - q_blocks) * COLS
        tail[k] = (total + kv_b[:, at : at + COLS]).astype(jnp.bfloat16)
        copy = put(tail.at[k], first + k)
        copy.start()
        copies.append(copy)
    for copy in copies:
        copy.wait()


def body(
    cache, payload, block_ids, block_counts, block_scales, refresh_ids, refresh_counts,
    norm_gain, query_weight, query_bias, kv_weight, kv_bias,
):
    rows, feature = cache.shape[1:]
    depth, q_cols = query_weight.shape[1:]
    kv_cols = kv_weight.shape[2]
    blocks = (q_cols + kv_cols) // COLS
    groups = blocks // GRP
    row_blocks = rows // BLK

    anywhere = pl.BlockSpec(memory_space=pl.ANY)
    vmem = pl.BlockSpec(memory_space=pltpu.VMEM)
    dma = pltpu.SemaphoreType.DMA
    held, outbuf, wlast, normed, partial = pl.pallas_call(
        kernel,
        out_shape=(
            pltpu.VMEM((rows, feature), jnp.bfloat16),
            pltpu.VMEM((blocks - GRP, rows, COLS), jnp.bfloat16),
            pltpu.VMEM((GRP, feature, COLS), jnp.bfloat16),
            pltpu.VMEM((rows, feature), jnp.bfloat16),
            pltpu.VMEM((GRP - 1, rows, COLS), jnp.float32),
        ),
        in_specs=[anywhere] * 12,
        out_specs=(vmem,) * 5,
        scratch_shapes=[
            pltpu.VMEM((blocks - GRP, feature, COLS), jnp.bfloat16),
            pltpu.VMEM((rows, feature), jnp.bfloat16),
            pltpu.VMEM((BLK, feature), jnp.bfloat16),
            pltpu.VMEM((BLK, feature), jnp.bfloat16),
            pltpu.VMEM((BLK, feature), jnp.bfloat16),
            pltpu.VMEM((8, BLK), jnp.int32),
            pltpu.VMEM((8, BLK), jnp.int32),
            pltpu.VMEM((1, q_cols + kv_cols), jnp.float32),
            dma((blocks,)),
            dma,
            dma((2,)),
            dma((CLASSES, groups)),
            dma((row_blocks,)),
            dma((row_blocks,)),
            dma,
            dma,
            pltpu.VMEM(block_ids.shape[1:], jnp.int32),
            pltpu.VMEM(block_counts.shape, jnp.int32),
            pltpu.VMEM(block_scales.shape[1:], jnp.int32),
            pltpu.VMEM(refresh_ids.shape[1:], jnp.int32),
            pltpu.VMEM(refresh_counts.shape, jnp.int32),
            pltpu.VMEM(norm_gain.shape, jnp.float32),
            dma((8,)),
            dma,
            dma,
            dma,
            dma,
            dma,
            dma,
        ],
        compiler_params=pltpu.CompilerParams(collective_id=0, has_side_effects=True, vmem_limit_bytes=38 * 1024 * 1024),
        name="boundary",
    )(
        cache[0], payload[0], block_ids[0], block_counts, block_scales[0], refresh_ids[0], refresh_counts,
        norm_gain, query_weight[0], query_bias, kv_weight[0], kv_bias,
    )
    rebuilt, queries, keys_values = pl.pallas_call(
        write,
        out_shape=tuple(jax.ShapeDtypeStruct((rows, n), jnp.bfloat16) for n in (feature, q_cols, kv_cols)),
        in_specs=[vmem] * 6,
        out_specs=(anywhere, anywhere, anywhere),
        scratch_shapes=[pltpu.VMEM((GRP, rows, COLS), jnp.bfloat16), dma((blocks + row_blocks,))],
        compiler_params=pltpu.CompilerParams(vmem_limit_bytes=4 * 1024 * 1024),
        name="write",
    )(held, outbuf, wlast, normed, partial, kv_bias)
    return rebuilt[None], queries[None], keys_values[None]


def solution(mesh):
    in_specs = (
        P("section", "rep", None),
        P("section", "rep", None),
        P("section", "rep", None),
        P("section", "rep"),
        P("section", "rep", None),
        P("section", "rep", None),
        P("section", "rep"),
        P("section", None),
        P("section", "rep", None),
        P("section", None),
        P("section", "rep", None),
        P("section", None),
    )
    out_specs = (P("section", "rep", None), P("section", "rep", None), P("section", "rep", None))
    return jax.shard_map(body, mesh=mesh, in_specs=in_specs, out_specs=out_specs, check_vma=False)
```
